128 devices in a mesh: gx: 16 (over y_lo, x, core), yz: 8 (over z, y_hi).
Axes of the slice: x: 4, y: 4 (y_hi: 2, y_lo: 2; y = y_hi * 2 + y_lo), z: 4, core: 2. Of those that a mesh axis runs over, the one named last changes fastest.
Arguments:
- vel: float32 [3, 96, 192, 1024], P(None, 'gx', 'yz'), may hold values from -6 to 6
- q_old: float32 [3, 96, 192, 1024], P(None, 'gx', None, 'yz'), may hold values from -6 to 6
- pressure_guess: float32 [96, 192, 1024], P('gx', None, 'yz'), may hold values from -6 to 6
- shear_shift: int32 [1], replicated, may hold values from 0 to 1023
Outputs:
- vel_next: float32 [3, 96, 192, 1024], P(None, 'gx', 'yz')
- q_next: float32 [3, 96, 192, 1024], P(None, 'gx', None, 'yz')
- pressure: float32 [96, 192, 1024], P('gx', None, 'yz')
The draws below stay inside these ranges and needn't reach their ends.
All inputs are finite; a program needn't handle non-finite values.
Results may differ from the reference program's by a relative error of at most 0.00013.
Values sent between devices are 32-bit elements; how exact they have to be, the bound alone decides.
A program may use at most 128 MiB of HBM per device.

```python
import math
import jax
import jax.numpy as jnp
from jax import lax

NY = 1024
NZ = 192
SWEEPS = 2
NX = 96
N_YZ = 8


def steps_of(rng, dims, cuts, smallest, top_value):
    def one(axis_at, shards_of):
        heights = jax.random.uniform(jax.random.fold_in(jax.random.fold_in(rng, 6), axis_at), (shards_of,), jnp.float32, smallest / len(cuts), top_value / len(cuts))
        return jnp.repeat(jnp.exp(heights), dims[axis_at] // shards_of).reshape((-1,) + (1,) * (len(dims) - axis_at - 1))

    factor_of = one(*cuts[0])
    for cut in cuts[1:]:
        factor_of = factor_of * one(*cut)
    return factor_of


def noise(key, extent, spread, bound, shards=(), kind=jnp.bfloat16):
    array = spread * jax.random.normal(key, extent, jnp.float32)
    if shards:
        array = array * steps_of(key, extent, shards, -0.22, 0.18)
    return jnp.clip(array, -bound, bound).astype(kind)


def setup_inputs(seed: int = 0) -> dict:
    streams_of = jax.random.split(jax.random.key(seed), 5)
    return {
        "vel": noise(streams_of[0], (3, NX, NZ, NY), 1.0, 6.0, ((1, 16), (2, 8)), jnp.float32),
        "q_old": noise(streams_of[1], (3, NX, NZ, NY), 1.0, 6.0, ((1, 16), (3, 8)), jnp.float32),
        "pressure_guess": noise(streams_of[2], (NX, NZ, NY), 1.0, 6.0, ((0, 16), (2, 8)), jnp.float32),
        "shear_shift": jax.random.randint(streams_of[3], (1,), 0, NY).astype(jnp.int32),
    }


highest = lax.Precision.HIGHEST
viscosity = 0.05
time_step = 0.2
keep_weight = -5.0 / 9.0
section_weight = 15.0 / 16.0
shear_param = 1.5
fraction = 0.375

def unpack(packed):
    leading = packed.shape[:-1]
    block_len = NY // (2 * N_YZ)
    viewed = packed.reshape(leading + (N_YZ, 2, block_len))
    return (viewed[..., 0, :].reshape(leading + (NY // 2,)), viewed[..., 1, :].reshape(leading + (NY // 2,)))

def pack(real_part, imag_part):
    leading = real_part.shape[:-1]
    block_len = NY // (2 * N_YZ)
    viewed = jnp.stack([real_part.reshape(leading + (N_YZ, block_len)), imag_part.reshape(leading + (N_YZ, block_len))], axis=-2)
    return viewed.reshape(leading + (NY,))

def x_slice(padded, offset):
    return padded[:, 3 + offset:3 + offset + NX]

def first_diff(padded):
    return (45.0 * (x_slice(padded, 1) - x_slice(padded, -1)) - 9.0 * (x_slice(padded, 2) - x_slice(padded, -2)) + (x_slice(padded, 3) - x_slice(padded, -3))) / 60.0

def second_diff(padded):
    return (2.0 * (x_slice(padded, 3) + x_slice(padded, -3)) - 27.0 * (x_slice(padded, 2) + x_slice(padded, -2)) + 270.0 * (x_slice(padded, 1) + x_slice(padded, -1)) - 490.0 * x_slice(padded, 0)) / 180.0

def rotate(real_part, imag_part, cosine, sine):
    return (real_part * cosine - imag_part * sine, real_part * sine + imag_part * cosine)

def reference(vel, q_old, pressure_guess, shear_shift):
    offset = shear_shift[0]
    tail_rows = vel[:, NX - 3:]
    front_rows = vel[:, :3]
    left_rim = (1.0 - fraction) * jnp.roll(tail_rows, -offset, axis=3) + fraction * jnp.roll(tail_rows, -offset - 1, axis=3)
    right_rim = (1.0 - fraction) * jnp.roll(front_rows, offset, axis=3) + fraction * jnp.roll(front_rows, offset + 1, axis=3)
    padded = jnp.concatenate([left_rim, vel, right_rim], axis=1)
    omega = 2.0 / NX
    xpos = jnp.arange(NX, dtype=jnp.int32).astype(jnp.float32) + 0.5 - NX / 2.0
    background = (-shear_param * omega * xpos)[:, None, None]
    coriolis = jnp.stack([2.0 * omega * vel[1], -(2.0 - shear_param) * omega * vel[0], jnp.zeros_like(vel[0])])
    term_a = -first_diff(padded * padded[0][None]) + viscosity * second_diff(padded) + coriolis
    term_b = -(vel[1] + background)[None] * vel
    term_c = -vel[2][None] * vel
    modes = jnp.arange(NY // 2, dtype=jnp.int32)
    cells_y = jnp.arange(NY, dtype=jnp.int32)
    angle_y = 2.0 * math.pi / NY * (cells_y[:, None] * modes[None, :] % NY).astype(jnp.float32)
    cos_y = jnp.cos(angle_y) / math.sqrt(NY)
    sin_y = jnp.sin(angle_y) / math.sqrt(NY)

    def y_forward(field):
        return (jnp.einsum('cxzy,yk->cxzk', field, cos_y, precision=highest), -jnp.einsum('cxzy,yk->cxzk', field, sin_y, precision=highest))
    ya_re, ya_im = y_forward(term_a)
    yb_re, yb_im = y_forward(term_b)
    yc_re, yc_im = y_forward(term_c)
    yu_re, yu_im = y_forward(vel)
    wave_y = 2.0 * math.pi / NY * modes.astype(jnp.float32)
    w_re = ya_re - wave_y * yb_im - viscosity * (wave_y * wave_y) * yu_re
    w_im = ya_im + wave_y * yb_re - viscosity * (wave_y * wave_y) * yu_im
    cells_z = jnp.arange(NZ, dtype=jnp.int32)
    angle_z = 2.0 * math.pi / NZ * (cells_z[:, None] * cells_z[None, :] % NZ).astype(jnp.float32)
    cos_z = jnp.cos(angle_z) / math.sqrt(NZ)
    sin_z = jnp.sin(angle_z) / math.sqrt(NZ)
    signed_z = jnp.where(cells_z < NZ // 2, cells_z, cells_z - NZ)
    wave_z = (2.0 * math.pi / NZ * signed_z.astype(jnp.float32))[:, None]

    def z_apply(real_part, imag_part, sign):
        cos_re = jnp.einsum('wz,cxzk->cxwk', cos_z, real_part, precision=highest)
        cos_im = jnp.einsum('wz,cxzk->cxwk', cos_z, imag_part, precision=highest)
        sin_re = jnp.einsum('wz,cxzk->cxwk', sin_z, real_part, precision=highest)
        sin_im = jnp.einsum('wz,cxzk->cxwk', sin_z, imag_part, precision=highest)
        return (cos_re + sign * sin_im, cos_im - sign * sin_re)
    zw_re, zw_im = z_apply(w_re, w_im, 1.0)
    zc_re, zc_im = z_apply(yc_re, yc_im, 1.0)
    zu_re, zu_im = z_apply(yu_re, yu_im, 1.0)
    tend_re = zw_re - wave_z * zc_im - viscosity * (wave_z * wave_z) * zu_re
    tend_im = zw_im + wave_z * zc_re - viscosity * (wave_z * wave_z) * zu_im
    edge_angle = 2.0 * math.pi / NY * ((modes * offset % NY).astype(jnp.float32) + fraction * modes.astype(jnp.float32))
    edge_cos = jnp.cos(edge_angle)
    edge_sin = jnp.sin(edge_angle)

    def neighbours(real_part, imag_part):
        low_re, low_im = rotate(real_part[NX - 1:], imag_part[NX - 1:], edge_cos, edge_sin)
        high_re, high_im = rotate(real_part[:1], imag_part[:1], edge_cos, -edge_sin)
        plus_re = jnp.concatenate([real_part[1:], high_re], axis=0)
        plus_im = jnp.concatenate([imag_part[1:], high_im], axis=0)
        minus_re = jnp.concatenate([low_re, real_part[:-1]], axis=0)
        minus_im = jnp.concatenate([low_im, imag_part[:-1]], axis=0)
        return (plus_re, plus_im, minus_re, minus_im)
    xp_re, xp_im, xm_re, xm_im = neighbours(tend_re[0], tend_im[0])
    div_re = 0.5 * (xp_re - xm_re) - wave_y * tend_im[1] - wave_z * tend_im[2]
    div_im = 0.5 * (xp_im - xm_im) + wave_y * tend_re[1] + wave_z * tend_re[2]
    denom = 2.0 + wave_y[None, :] * wave_y[None, :] + wave_z * wave_z
    press_re, press_im = unpack(pressure_guess)
    for sweep_no in range(SWEEPS):
        pp_re, pp_im, pm_re, pm_im = neighbours(press_re, press_im)
        press_re = (pp_re + pm_re - div_re) / denom
        press_im = (pp_im + pm_im - div_im) / denom
    pp_re, pp_im, pm_re, pm_im = neighbours(press_re, press_im)
    grad_re = jnp.stack([0.5 * (pp_re - pm_re), -wave_y * press_im, -wave_z * press_im])
    grad_im = jnp.stack([0.5 * (pp_im - pm_im), wave_y * press_re, wave_z * press_re])
    old_re, old_im = unpack(q_old)
    new_re = keep_weight * old_re + time_step * (tend_re - grad_re)
    new_im = keep_weight * old_im + time_step * (tend_im - grad_im)
    q_next = pack(new_re, new_im)
    back_re, back_im = z_apply(new_re, new_im, -1.0)
    weights = jnp.where(modes == 0, 1.0, 2.0).astype(jnp.float32)
    correction = jnp.einsum('cxzk,yk->cxzy', back_re, cos_y * weights[None, :], precision=highest) - jnp.einsum('cxzk,yk->cxzy', back_im, sin_y * weights[None, :], precision=highest)
    vel_next = vel + section_weight * correction
    return (vel_next, q_next, pack(press_re, press_im))
```

```python
import functools
import math

import jax
import jax.numpy as jnp
import numpy as np
from jax import lax
from jax.experimental import pallas as pl
from jax.experimental.pallas import tpu as pltpu
from jax.sharding import PartitionSpec as P

viscosity = 0.05
time_step = 0.2
keep_weight = -5.0 / 9.0
section_weight = 15.0 / 16.0
shear_param = 1.5
fraction = 0.375
GROUPS = 8
MESH = pl.DeviceIdType.MESH
F32 = jnp.float32
BF16 = jnp.bfloat16


def tables(width_y, depth_z):
    half = width_y // (2 * GROUPS)
    lanes = np.arange(width_y)
    mode = lanes // (2 * half) * half + lanes % half
    is_im = (lanes // half) % 2 == 1
    coarse = np.arange(width_y // half)
    fine = np.arange(half)

    def angle(n, k):
        return 2.0 * np.pi / width_y * ((n[:, None] * k[None, :]) % width_y)

    scale = 1.0 / math.sqrt(width_y)
    alpha = angle(coarse * half, mode)
    beta = angle(fine, mode)
    fwd_coarse = np.concatenate([np.cos(alpha), np.sin(alpha)])
    fwd_fine = scale * np.stack(
        [
            np.where(is_im[None], -np.sin(beta), np.cos(beta)),
            np.where(is_im[None], -np.cos(beta), -np.sin(beta)),
        ]
    )
    cells = np.arange(width_y)
    alpha = angle(np.arange(GROUPS) * half, cells)
    beta = angle(fine, cells)
    inv_coarse = np.concatenate([np.cos(alpha), np.sin(alpha)])
    inv_fine = (2.0 * section_weight * scale) * np.stack(
        [
            np.concatenate([np.cos(beta), -np.sin(beta)]),
            np.concatenate([-np.sin(beta), -np.cos(beta)]),
        ]
    )
    wave_y = 2.0 * np.pi / width_y * mode[None, :]
    m = np.arange(depth_z)
    signed = np.where(m < depth_z // 2, m, m - depth_z)
    wave_z = (2.0 * np.pi / depth_z * signed)[:, None]
    angle_z = 2.0 * np.pi / depth_z * ((m[:, None] * m[None, :]) % depth_z)
    forward = np.exp(-1j * angle_z) / math.sqrt(depth_z)
    mats = [
        forward,
        1j * wave_z * forward,
        -viscosity * wave_z * wave_z * forward,
        np.exp(1j * angle_z) / math.sqrt(depth_z),
    ]
    stacked = []
    for mat in mats:
        both = np.concatenate([mat.real, mat.imag]).astype(np.float32)
        high = both.astype(BF16)
        low = (both - high.astype(np.float32)).astype(BF16)
        stacked.append(np.concatenate([high, low]))
    as32 = lambda v: jnp.asarray(np.asarray(v, np.float32))
    return (
        as32(fwd_coarse),
        as32(fwd_fine),
        as32(inv_coarse),
        as32(inv_fine),
        as32(wave_y),
        as32(np.broadcast_to(wave_z, (depth_z, 2 * half))),
        jnp.asarray(np.stack(stacked)),
    )


def split(value):
    high = value.astype(BF16)
    low = (value - high.astype(F32)).astype(BF16)
    return high, low


def mm(a, b):
    return jnp.dot(a, b, preferred_element_type=F32)


def body(
    slabs,
    shift_ref,
    vel_hbm,
    qold_hbm,
    guess_hbm,
    edge_hbm,
    fcoarse_hbm,
    ffine_hbm,
    icoarse_hbm,
    ifine_hbm,
    wavey_hbm,
    wavez_hbm,
    zmat_hbm,
    vnext_hbm,
    qnext_hbm,
    pout_hbm,
    ghost,
    fcoarse,
    ffine,
    icoarse,
    ifine,
    wavey,
    wavez,
    zmat,
    edge,
    qold,
    f_hi,
    f_lo,
    l_hi,
    l_lo,
    spec_u,
    spec_c,
    spec_w,
    got_u,
    got_c,
    got_w,
    tend,
    tend_x,
    cross,
    guess,
    recip,
    press,
    spatial,
    got_s,
    load_sem,
    halo_send,
    halo_recv,
    fwd_send,
    fwd_recv,
    inv_send,
    inv_recv,
    out_sem,
):
    gx = lax.axis_index("gx")
    me = lax.axis_index("yz")
    my_z = me // 2
    right = lax.rem(gx + 1, slabs)
    left = lax.rem(gx + slabs - 1, slabs)
    planes = 6
    rows = 24
    width = 1024
    depth = 192
    lanes = 128
    half = 64
    flat = planes * rows * 3

    def peer(d):
        return lax.rem(me + d, GROUPS)

    loads = [
        (vel_hbm, ghost.at[:, pl.ds(3, planes)]),
        (fcoarse_hbm, fcoarse),
        (ffine_hbm, ffine),
        (guess_hbm, guess.at[pl.ds(3, planes)]),
        (wavey_hbm, wavey),
        (edge_hbm, edge),
        (zmat_hbm, zmat),
        (wavez_hbm, wavez),
        (icoarse_hbm, icoarse),
        (ifine_hbm, ifine),
        (qold_hbm, qold),
    ]
    loads = [pltpu.make_async_copy(s, d, load_sem.at[i]) for i, (s, d) in enumerate(loads)]
    for copy in loads:
        copy.start()

    barrier = pltpu.get_barrier_semaphore()
    for d in range(1, GROUPS):
        pl.semaphore_signal(
            barrier, inc=1, device_id={"gx": gx, "yz": peer(d)}, device_id_type=MESH
        )
    for side in (left, right):
        pl.semaphore_signal(barrier, inc=1, device_id={"gx": side, "yz": me}, device_id_type=MESH)

    def halo(ref, count, own, slot, lead):
        def at(start):
            return ref.at[:, pl.ds(start, count)] if lead else ref.at[pl.ds(start, count)]

        to_left = pltpu.make_async_remote_copy(
            src_ref=at(count), dst_ref=at(count + own), send_sem=halo_send.at[slot],
            recv_sem=halo_recv.at[slot], device_id={"gx": left, "yz": me}, device_id_type=MESH,
        )
        to_right = pltpu.make_async_remote_copy(
            src_ref=at(own), dst_ref=at(0), send_sem=halo_send.at[slot + 1],
            recv_sem=halo_recv.at[slot + 1], device_id={"gx": right, "yz": me}, device_id_type=MESH,
        )
        return to_left, to_right

    loads[0].wait()
    loads[3].wait()
    pl.semaphore_wait(barrier, GROUPS + 1)
    vel_halo = halo(ghost, 3, planes, 0, True)
    guess_halo = halo(guess, 3, planes, 2, False)
    for copy in vel_halo + guess_halo:
        copy.start()

    def store_split(at, value):
        high, low = split(value)
        where = pl.ds(pl.multiple_of(at, 48), 48)
        l_hi[where, :] = high
        l_lo[where, :] = low

    def build(dst_hi, dst_lo, coarse, fine, steps, length):
        def step(a, carry):
            value = (
                coarse[pl.ds(a, 1), :] * fine[0] + coarse[pl.ds(a + steps, 1), :] * fine[1]
            )
            high, low = split(value)
            where = pl.ds(pl.multiple_of(a * length, length), length)
            dst_hi[where, :] = high
            dst_lo[where, :] = low
            return carry

        lax.fori_loop(0, steps, step, 0)

    def pairs_loop(write):
        def step(i, carry):
            write(i // 3, lax.rem(i, 3) * 2, i * 48)
            return carry

        lax.fori_loop(0, 9, step, 0)

    def put_u(c, p, at):
        store_split(at, ghost[c, pl.ds(3 + p, 2)].reshape(48, width))

    loads[1].wait()
    loads[2].wait()
    build(f_hi, f_lo, fcoarse, ffine, width // half, half)
    pairs_loop(put_u)

    def to_modes(at, col):
        a_hi = l_hi[pl.ds(at, flat), :]
        a_lo = l_lo[pl.ds(at, flat), :]
        b_hi = f_hi[:, pl.ds(col, 256)]
        b_lo = f_lo[:, pl.ds(col, 256)]
        return mm(a_hi, b_hi) + mm(a_lo, b_hi) + mm(a_hi, b_lo)

    def fwd_copy(spec, got, kind, dest, first, count):
        return pltpu.make_async_remote_copy(
            src_ref=spec.at[pl.ds(first, count), :, pl.ds(pl.multiple_of(dest * lanes, lanes), lanes)],
            dst_ref=got.at[pl.ds(first, count), pl.ds(pl.multiple_of(me * rows, 8), rows), :],
            send_sem=fwd_send.at[kind, dest],
            recv_sem=fwd_recv.at[kind, me],
            device_id={"gx": gx, "yz": dest},
            device_id_type=MESH,
        )

    def fwd_own(spec, got, kind, first, count):
        return pltpu.make_async_copy(
            spec.at[pl.ds(first, count), :, pl.ds(pl.multiple_of(me * lanes, lanes), lanes)],
            got.at[pl.ds(first, count), pl.ds(pl.multiple_of(me * rows, 8), rows), :],
            fwd_recv.at[kind, me],
        )

    def fwd_wait(got, kind, first, count):
        def step(d, carry):
            src = peer(d)
            pltpu.make_async_remote_copy(
                src_ref=got.at[pl.ds(first, count), pl.ds(pl.multiple_of(src * rows, 8), rows), :],
                dst_ref=got.at[pl.ds(first, count), pl.ds(pl.multiple_of(src * rows, 8), rows), :],
                send_sem=fwd_send.at[kind, src],
                recv_sem=fwd_recv.at[kind, src],
                device_id={"gx": gx, "yz": src},
                device_id_type=MESH,
            ).wait_recv()
            return carry

        lax.fori_loop(1, GROUPS, step, 0)

    partner = me + 1 - 2 * lax.rem(me, 2)

    def transform_and_send(spec, got, kind):
        def step(i, carry):
            target = lax.rem(my_z + 1 + i, 4)
            col = pl.multiple_of(target * 256, 256)
            spec[:, :, pl.ds(col, 256)] = to_modes(0, col).reshape(18, rows, 256)
            for side in range(2):
                dest = target * 2 + side

                @pl.when(dest != me)
                def _():
                    fwd_copy(spec, got, kind, dest, 0, 18).start()

            return carry

        lax.fori_loop(0, 4, step, 0)
        fwd_own(spec, got, kind, 0, 18).start()

    transform_and_send(spec_u, got_u, 0)

    def put_c(c, p, at):
        u_z = ghost[2, pl.ds(3 + p, 2)]
        store_split(at, (-u_z * ghost[c, pl.ds(3 + p, 2)]).reshape(48, width))

    pairs_loop(put_c)
    transform_and_send(spec_c, got_c, 1)

    for copy in vel_halo:
        copy.wait_recv()
    shift = shift_ref[0]

    def moved(value, amount, extra):
        once = pltpu.roll(value, amount, 1)
        return (1.0 - fraction) * once + fraction * pltpu.roll(once, extra, 1)

    def fix(start, amount, extra):
        def step(i, carry):
            c, p = i // 3, lax.rem(i, 3) + start
            ghost[c, p] = moved(ghost[c, p], amount, extra)
            return carry

        lax.fori_loop(0, 9, step, 0)

    @pl.when(gx == 0)
    def _():
        fix(0, lax.rem(width - shift, width), width - 1)

    @pl.when(gx == slabs - 1)
    def _():
        fix(planes + 3, shift, 1)

    total_x = planes * slabs
    omega = 2.0 / total_x

    def put_ab(i, carry):
        c, p = i // 3, lax.rem(i, 3) * 2
        terms_a = []
        terms_b = []
        for q in range(2):
            at = p + q + 3
            u_x = [ghost[0, at + o] for o in range(-3, 4)]
            u_i = [ghost[c, at + o] for o in range(-3, 4)]
            prod = [x * y for x, y in zip(u_x, u_i)]
            first = (
                (45.0 / 60.0) * (prod[4] - prod[2])
                - (9.0 / 60.0) * (prod[5] - prod[1])
                + (1.0 / 60.0) * (prod[6] - prod[0])
            )
            second = (
                (2.0 / 180.0) * (u_i[6] + u_i[0])
                - (27.0 / 180.0) * (u_i[5] + u_i[1])
                + (270.0 / 180.0) * (u_i[4] + u_i[2])
                - (490.0 / 180.0) * u_i[3]
            )
            u_y = ghost[1, at]
            weight_y = jnp.where(c == 0, 2.0 * omega, 0.0).astype(F32)
            weight_x = jnp.where(c == 1, -(2.0 - shear_param) * omega, 0.0).astype(F32)
            terms_a.append(viscosity * second - first + (weight_y * u_y + weight_x * u_x[3]))
            place = (gx * planes + p + q).astype(F32) + 0.5 - total_x / 2.0
            background = -shear_param * omega * place
            terms_b.append(-(u_y + background) * u_i[3])
        store_split(i * 48, jnp.concatenate(terms_a, axis=0))
        store_split(flat + i * 48, jnp.concatenate(terms_b, axis=0))
        return carry

    lax.fori_loop(0, 9, put_ab, 0)

    loads[4].wait()
    sign = jnp.where(lax.broadcasted_iota(jnp.int32, (1, lanes), 1) < half, -1.0, 1.0).astype(F32)

    def turned(value):
        return pltpu.roll(value, half, 1) * sign

    def combine(i, carry):
        target = lax.rem(my_z + 1 + i, 4)
        col = pl.multiple_of(target * 256, 256)
        ya = to_modes(0, col)
        yb = to_modes(flat, col)
        for side in range(2):
            wide = pl.ds(pl.multiple_of(col + side * lanes, lanes), lanes)
            cut = slice(side * lanes, (side + 1) * lanes)
            ky = wavey[0:1, wide]
            yu = spec_u[:, :, wide].reshape(flat, lanes)
            out = ya[:, cut] + turned(yb[:, cut]) * ky - (viscosity * ky * ky) * yu
            spec_w[:, :, wide] = out.reshape(18, rows, lanes)
        return carry

    lax.fori_loop(0, 4, combine, 0)
    for c in range(3):
        def send(i, carry, c=c):
            target = lax.rem(my_z + 1 + i, 4)
            for side in range(2):
                dest = target * 2 + side

                @pl.when(dest != me)
                def _():
                    fwd_copy(spec_w, got_w, 2 + c, dest, c * planes, planes).start()

            return carry

        lax.fori_loop(0, 4, send, 0)
        fwd_own(spec_w, got_w, 2 + c, c * planes, planes).start()

    loads[5].wait()
    loads[6].wait()
    loads[7].wait()
    own_ky = wavey[0:1, pl.ds(pl.multiple_of(me * lanes, lanes), lanes)]
    recip[...] = 1.0 / (2.0 + own_ky * own_ky + wavez[...] * wavez[...])

    def rotate_ends(ref, count, own):
        cosine = edge[0:1, :]
        sine = edge[1:2, :]

        @pl.when(gx == 0)
        def _():
            for j in range(count):
                value = ref[j]
                ref[j] = value * cosine + turned(value) * sine

        @pl.when(gx == slabs - 1)
        def _():
            for j in range(own + count, own + 2 * count):
                value = ref[j]
                ref[j] = value * cosine - turned(value) * sine

    for copy in guess_halo:
        copy.wait_recv()
    rotate_ends(guess, 3, planes)

    def z_pair(ref, at, kind):
        value = jnp.concatenate([ref[at], ref[at + 1]], axis=1)
        high, low = split(value)
        mat = zmat[kind]
        return mm(mat, high), mm(zmat[kind, pl.ds(0, 2 * depth)], low)

    def z_join(parts):
        total = sum(wide[: 2 * depth] + wide[2 * depth :] + low for wide, low in parts)
        out = []
        for q in range(2):
            cut = slice(q * lanes, (q + 1) * lanes)
            out.append(total[:depth, cut] + turned(total[depth:, cut]))
        return out

    for copy in (fwd_own(spec_u, got_u, 0, 0, 18), fwd_own(spec_c, got_c, 1, 0, 18)):
        copy.wait()
    fwd_wait(got_u, 0, 0, 18)
    fwd_wait(got_c, 1, 0, 18)

    def z_first(i, carry):
        at = i * 2
        first, second = z_join([z_pair(got_c, at, 1), z_pair(got_u, at, 2)])
        tend[at] = first
        tend[at + 1] = second
        return carry

    lax.fori_loop(0, 9, z_first, 0)

    loads[8].wait()
    loads[9].wait()
    build(f_hi, f_lo, icoarse, ifine, GROUPS, 2 * half)
    head_hi = f_hi[0:16, :]
    head_lo = f_lo[0:16, :]
    top = lax.broadcasted_iota(jnp.int32, (16, width), 0) == 0
    f_hi[0:16, :] = jnp.where(top, head_hi.astype(F32) * 0.5, head_hi.astype(F32)).astype(BF16)
    f_lo[0:16, :] = jnp.where(top, head_lo.astype(F32) * 0.5, head_lo.astype(F32)).astype(BF16)

    def z_last(c, write):
        fwd_own(spec_w, got_w, 2 + c, c * planes, planes).wait()
        fwd_wait(got_w, 2 + c, c * planes, planes)

        def step(i, carry):
            at = c * planes + i * 2
            values = z_join([z_pair(got_w, at, 0)])
            for q in range(2):
                write(i * 2 + q, at + q, tend[at + q] + values[q])
            return carry

        lax.fori_loop(0, 3, step, 0)

    def write_x(p, at, value):
        tend[at] = value
        tend_x[p + 3] = value

    z_last(0, write_x)
    x_halo = halo(tend_x, 3, planes, 4, False)
    for copy in x_halo:
        copy.start()

    def write_y(p, at, value):
        tend[at] = value
        cross[p + 2] = turned(value) * own_ky

    z_last(1, write_y)

    def write_z(p, at, value):
        tend[at] = value
        cross[p + 2] = cross[p + 2] + turned(value) * wavez[...]

    z_last(2, write_z)
    cross_halo = halo(cross, 2, planes, 6, False)
    for copy in cross_halo:
        copy.start()
    loads[10].wait()
    for copy in x_halo:
        copy.wait_recv()
    rotate_ends(tend_x, 3, planes)
    for copy in cross_halo:
        copy.wait_recv()
    rotate_ends(cross, 2, planes)

    def diverge(j, carry):
        got_u[j] = 0.5 * (tend_x[j + 2] - tend_x[j]) + cross[j]
        return carry

    lax.fori_loop(0, planes + 4, diverge, 0)

    def sweep_a(j, carry):
        got_c[j] = (guess[j + 2] + guess[j] - got_u[j]) * recip[...]
        return carry

    lax.fori_loop(0, planes + 4, sweep_a, 0)

    def sweep_b(j, carry):
        press[j] = (got_c[j + 2] + got_c[j] - got_u[j + 1]) * recip[...]
        return carry

    lax.fori_loop(0, planes + 2, sweep_b, 0)
    pltpu.make_async_copy(press.at[pl.ds(1, planes)], pout_hbm, out_sem.at[0]).start()

    def inv_copy(c, dest):
        return pltpu.make_async_remote_copy(
            src_ref=spatial.at[pl.ds(c * planes, planes), pl.ds(pl.multiple_of(dest * rows, 8), rows), :],
            dst_ref=got_s.at[pl.ds(c * planes, planes), :, pl.ds(pl.multiple_of(me * lanes, lanes), lanes)],
            send_sem=inv_send.at[c, dest],
            recv_sem=inv_recv.at[c, me],
            device_id={"gx": gx, "yz": dest},
            device_id_type=MESH,
        )

    def inv_own(c):
        return pltpu.make_async_copy(
            spatial.at[pl.ds(c * planes, planes), pl.ds(pl.multiple_of(me * rows, 8), rows), :],
            got_s.at[pl.ds(c * planes, planes), :, pl.ds(pl.multiple_of(me * lanes, lanes), lanes)],
            inv_recv.at[c, me],
        )

    for c in range(3):
        def update(p, carry, c=c):
            at = c * planes + p
            here = press[p + 1]
            if c == 0:
                slope = 0.5 * (press[p + 2] - press[p])
            elif c == 1:
                slope = turned(here) * own_ky
            else:
                slope = turned(here) * wavez[...]
            qold[c, p] = keep_weight * qold[c, p] + time_step * (tend[at] - slope)
            return carry

        lax.fori_loop(0, planes, update, 0)

        def back(i, carry, c=c):
            at = c * planes + i * 2
            values = z_join([z_pair(qold.at[c], i * 2, 3)])
            spatial[at] = values[0]
            spatial[at + 1] = values[1]
            return carry

        lax.fori_loop(0, 3, back, 0)

        def send(i, carry, c=c):
            inv_copy(c, peer(i)).start()
            return carry

        lax.fori_loop(1, GROUPS, send, 0)
        inv_own(c).start()
    pltpu.make_async_copy(qold, qnext_hbm, out_sem.at[1]).start()

    rows_c = planes * rows
    for c in range(3):
        inv_own(c).wait()

        def arrive(d, carry, c=c):
            src = peer(d)
            where = got_s.at[pl.ds(c * planes, planes), :, pl.ds(pl.multiple_of(src * lanes, lanes), lanes)]
            pltpu.make_async_remote_copy(
                src_ref=where, dst_ref=where, send_sem=inv_send.at[c, src],
                recv_sem=inv_recv.at[c, src], device_id={"gx": gx, "yz": src}, device_id_type=MESH,
            ).wait_recv()
            return carry

        lax.fori_loop(1, GROUPS, arrive, 0)
        high, low = split(got_s[pl.ds(c * planes, planes)].reshape(rows_c, width))
        l_hi[pl.ds(c * rows_c, rows_c), :] = high
        l_lo[pl.ds(c * rows_c, rows_c), :] = low

        def step(i, carry, c=c):
            cols = pl.ds(pl.multiple_of(i * 256, 256), 256)
            a_hi = l_hi[pl.ds(c * rows_c, rows_c), :]
            a_lo = l_lo[pl.ds(c * rows_c, rows_c), :]
            out = mm(a_hi, f_hi[:, cols]) + mm(a_lo, f_hi[:, cols]) + mm(a_hi, f_lo[:, cols])
            spec_u[pl.ds(c * planes, planes), :, cols] = (
                ghost[c, pl.ds(3, planes), :, cols] + out.reshape(planes, rows, 256)
            )
            return carry

        if c == 0:
            def sent(d, carry):
                fwd_copy(spec_u, got_u, 0, peer(d), 0, 18).wait_send()
                return carry

            lax.fori_loop(1, GROUPS, sent, 0)
        lax.fori_loop(0, 4, step, 0)
        pltpu.make_async_copy(
            spec_u.at[pl.ds(c * planes, planes)], vnext_hbm.at[c], out_sem.at[2 + c]
        ).start()

    def drain(d, carry):
        dest = peer(d)
        fwd_copy(spec_c, got_c, 1, dest, 0, 18).wait_send()
        for c in range(3):
            fwd_copy(spec_w, got_w, 2 + c, dest, c * planes, planes).wait_send()
            inv_copy(c, dest).wait_send()
        return carry

    lax.fori_loop(1, GROUPS, drain, 0)
    for copy in vel_halo + guess_halo + x_halo + cross_halo:
        copy.wait_send()
    pltpu.make_async_copy(press.at[pl.ds(1, planes)], pout_hbm, out_sem.at[0]).wait()
    pltpu.make_async_copy(qold, qnext_hbm, out_sem.at[1]).wait()
    for c in range(3):
        pltpu.make_async_copy(
            spec_u.at[pl.ds(c * planes, planes)], vnext_hbm.at[c], out_sem.at[2 + c]
        ).wait()


def local(slabs, vel, q_old, pressure_guess, shear_shift):
    width = vel.shape[3]
    depth = q_old.shape[2]
    half = width // (2 * GROUPS)
    planes, rows = vel.shape[1], vel.shape[2]
    consts = tables(width, depth)
    modes = lax.axis_index("yz") * half + jnp.arange(2 * half, dtype=jnp.int32) % half
    angle = (2.0 * math.pi / width) * (
        (modes * shear_shift[0] % width).astype(F32) + fraction * modes.astype(F32)
    )
    edge = jnp.stack([jnp.cos(angle), jnp.sin(angle)])
    any_spec = pl.BlockSpec(memory_space=pl.ANY)
    vmem = lambda *shape: pltpu.VMEM(shape, F32)
    wide = lambda n: pltpu.VMEM((n, depth, 2 * half), F32)
    flat = 3 * planes * rows
    scratch = [
        vmem(3, planes + 6, rows, width),
        vmem(*consts[0].shape),
        vmem(*consts[1].shape),
        vmem(*consts[2].shape),
        vmem(*consts[3].shape),
        vmem(*consts[4].shape),
        vmem(*consts[5].shape),
        pltpu.VMEM(consts[6].shape, BF16),
        vmem(2, 2 * half),
        vmem(3, planes, depth, 2 * half),
        pltpu.VMEM((width, width), BF16),
        pltpu.VMEM((width, width), BF16),
        pltpu.VMEM((2 * flat, width), BF16),
        pltpu.VMEM((2 * flat, width), BF16),
        vmem(3 * planes, rows, width),
        vmem(3 * planes, rows, width),
        vmem(3 * planes, rows, width),
        wide(3 * planes),
        wide(3 * planes),
        wide(3 * planes),
        wide(3 * planes),
        wide(planes + 6),
        wide(planes + 4),
        wide(planes + 6),
        vmem(depth, 2 * half),
        wide(planes + 2),
        wide(3 * planes),
        vmem(3 * planes, rows, width),
        pltpu.SemaphoreType.DMA((11,)),
        pltpu.SemaphoreType.DMA((8,)),
        pltpu.SemaphoreType.DMA((8,)),
        pltpu.SemaphoreType.DMA((5, GROUPS)),
        pltpu.SemaphoreType.DMA((5, GROUPS)),
        pltpu.SemaphoreType.DMA((3, GROUPS)),
        pltpu.SemaphoreType.DMA((3, GROUPS)),
        pltpu.SemaphoreType.DMA((5,)),
    ]
    call = pl.pallas_call(
        functools.partial(body, slabs),
        out_shape=(
            jax.ShapeDtypeStruct(vel.shape, F32),
            jax.ShapeDtypeStruct(q_old.shape, F32),
            jax.ShapeDtypeStruct(pressure_guess.shape, F32),
        ),
        in_specs=[pl.BlockSpec(memory_space=pltpu.SMEM)] + [any_spec] * 11,
        out_specs=(any_spec, any_spec, any_spec),
        scratch_shapes=scratch,
        compiler_params=pltpu.CompilerParams(
            collective_id=0, has_side_effects=True, vmem_limit_bytes=63 * 2**20
        ),
        name="section",
    )
    return call(shear_shift, vel, q_old, pressure_guess, edge, *consts)


def solution(mesh):
    in_specs = (P(None, "gx", "yz", None), P(None, "gx", None, "yz"), P("gx", None, "yz"), P())
    out_specs = (P(None, "gx", "yz", None), P(None, "gx", None, "yz"), P("gx", None, "yz"))
    return jax.shard_map(
        functools.partial(local, mesh.shape["gx"]),
        mesh=mesh, in_specs=in_specs, out_specs=out_specs, check_vma=False,
    )
```

```python
import functools
import math

import jax
import jax.numpy as jnp
import numpy as np
from jax import lax
from jax.experimental import pallas as pl
from jax.experimental.pallas import tpu as pltpu
from jax.sharding import PartitionSpec as P

viscosity = 0.05
time_step = 0.2
keep_weight = -5.0 / 9.0
section_weight = 15.0 / 16.0
shear_param = 1.5
fraction = 0.375
GROUPS = 8
MESH = pl.DeviceIdType.MESH
F32 = jnp.float32
BF16 = jnp.bfloat16


def tables(width_y, depth_z):
    half = width_y // (2 * GROUPS)
    lanes = np.arange(width_y)
    mode = lanes // (2 * half) * half + lanes % half
    is_im = (lanes // half) % 2 == 1
    coarse = np.arange(width_y // half)
    fine = np.arange(half)

    def angle(n, k):
        return 2.0 * np.pi / width_y * ((n[:, None] * k[None, :]) % width_y)

    scale = 1.0 / math.sqrt(width_y)
    alpha = angle(coarse * half, mode)
    beta = angle(fine, mode)
    fwd_coarse = np.concatenate([np.cos(alpha), np.sin(alpha)])
    fwd_fine = scale * np.where(is_im[None], -np.sin(beta), np.cos(beta))
    cells = np.arange(width_y)
    alpha = angle(np.arange(GROUPS) * half, cells)
    beta = angle(fine, cells)
    inv_coarse = np.concatenate([np.cos(alpha), np.sin(alpha)])
    inv_fine = (2.0 * section_weight * scale) * np.stack([np.cos(beta), -np.sin(beta)])
    wave_y = 2.0 * np.pi / width_y * mode[None, :]
    m = np.arange(depth_z)
    signed = np.where(m < depth_z // 2, m, m - depth_z)
    wave_z = (2.0 * np.pi / depth_z * signed)[:, None]
    angle_z = 2.0 * np.pi / depth_z * ((m[:, None] * m[None, :]) % depth_z)
    forward = np.exp(-1j * angle_z) / math.sqrt(depth_z)
    mats = [
        forward,
        1j * wave_z * forward,
        -viscosity * wave_z * wave_z * forward,
        np.exp(1j * angle_z) / math.sqrt(depth_z),
    ]
    stacked = []
    for mat in mats:
        both = np.concatenate([mat.real, mat.imag]).astype(np.float32)
        high = both.astype(BF16)
        low = (both - high.astype(np.float32)).astype(BF16)
        stacked.append(np.concatenate([high, low]))
    as32 = lambda v: jnp.asarray(np.asarray(v, np.float32))
    return (
        as32(fwd_coarse),
        as32(fwd_fine),
        as32(inv_coarse),
        as32(inv_fine),
        as32(wave_y),
        as32(np.broadcast_to(wave_z, (depth_z, 2 * half))),
        jnp.asarray(np.stack(stacked)),
    )


def split(value):
    high = value.astype(BF16)
    low = (value - high.astype(F32)).astype(BF16)
    return high, low


def mm(a, b):
    return jnp.dot(a, b, preferred_element_type=F32)


def body(
    slabs,
    shift_ref,
    vel_hbm,
    qold_hbm,
    guess_hbm,
    edge_hbm,
    fcoarse_hbm,
    ffine_hbm,
    icoarse_hbm,
    ifine_hbm,
    wavey_hbm,
    wavez_hbm,
    zmat_hbm,
    vnext,
    qnext,
    pout,
    ghost,
    fcoarse,
    ffine,
    icoarse,
    ifine,
    wavey,
    wavez,
    zmat,
    edge,
    qold,
    f_hi,
    f_lo,
    left_side,
    spec_u,
    spec_c,
    spec_w,
    got_u,
    got_c,
    got_w,
    tend,
    tend_x,
    cross,
    guess,
    late,
    recip,
    diverge,
    first,
    press,
    spatial,
    got_s,
    load_sem,
    halo_send,
    halo_recv,
    fwd_send,
    fwd_recv,
    inv_send,
    inv_recv,
):
    gx = lax.axis_index("gx")
    me = lax.axis_index("yz")
    my_z = me // 2
    right = lax.rem(gx + 1, slabs)
    left = lax.rem(gx + slabs - 1, slabs)
    planes = 6
    rows = 24
    width = 1024
    depth = 192
    lanes = 128
    half = 64
    flat = planes * rows * 3

    def peer(d):
        return lax.rem(me + d, GROUPS)

    def own_cols(ref_index):
        return pl.ds(pl.multiple_of(ref_index * lanes, lanes), lanes)

    def own_rows(ref_index):
        return pl.ds(pl.multiple_of(ref_index * rows, 8), rows)

    loads = [
        (vel_hbm, ghost.at[:, pl.ds(3, planes)]),
        (fcoarse_hbm, fcoarse),
        (ffine_hbm, ffine.at[0]),
        (guess_hbm, guess.at[pl.ds(2, planes)]),
        (wavey_hbm, wavey),
        (edge_hbm, edge),
        (zmat_hbm, zmat),
        (wavez_hbm, wavez),
        (icoarse_hbm, icoarse),
        (ifine_hbm, ifine),
        (qold_hbm, qold),
    ]
    loads = [pltpu.make_async_copy(s, d, load_sem.at[i]) for i, (s, d) in enumerate(loads)]
    for i in (1, 2, 0, 3, 4, 5, 6, 7, 8, 9, 10):
        loads[i].start()

    barrier = pltpu.get_barrier_semaphore()
    for d in range(1, GROUPS):
        pl.semaphore_signal(
            barrier, inc=1, device_id={"gx": gx, "yz": peer(d)}, device_id_type=MESH
        )
    for side in (left, right):
        pl.semaphore_signal(barrier, inc=1, device_id={"gx": side, "yz": me}, device_id_type=MESH)

    def x_copy(src, dst, slot, target):
        return pltpu.make_async_remote_copy(
            src_ref=src, dst_ref=dst, send_sem=halo_send.at[slot], recv_sem=halo_recv.at[slot],
            device_id={"gx": target, "yz": me}, device_id_type=MESH,
        )

    def halo(ref, count, slot, lead):
        def at(start):
            return ref.at[:, pl.ds(start, count)] if lead else ref.at[pl.ds(start, count)]

        return (
            x_copy(at(count), at(count + planes), slot, left),
            x_copy(at(planes), at(0), slot + 1, right),
        )

    sign = jnp.where(lax.broadcasted_iota(jnp.int32, (1, lanes), 1) < half, -1.0, 1.0).astype(F32)

    def turned(value):
        return pltpu.roll(value, half, 1) * sign

    def store_split(at, value, gap=flat):
        high, low = split(value)
        left_side[pl.ds(pl.multiple_of(at, 48), 48), :] = high
        left_side[pl.ds(pl.multiple_of(at + gap, 48), 48), :] = low

    def build(col):
        cols = pl.ds(col, 256)
        for side in range(2):
            part = pl.ds(pl.multiple_of(col + side * lanes, lanes), lanes)
            ffine[1, :, part] = -turned(ffine[0, :, part])

        def step(a, carry):
            value = (
                fcoarse[pl.ds(a, 1), cols] * ffine[0, :, cols]
                + fcoarse[pl.ds(a + width // half, 1), cols] * ffine[1, :, cols]
            )
            high, low = split(value)
            where = pl.ds(pl.multiple_of(a * half, half), half)
            f_hi[where, cols] = high
            f_lo[where, cols] = low
            return carry

        lax.fori_loop(0, width // half, step, 0)

    def pairs_loop(write):
        def step(i, carry):
            write(i // 3, lax.rem(i, 3) * 2, i * 48)
            return carry

        lax.fori_loop(0, 9, step, 0)

    def to_modes(slot, col):
        cols = pl.ds(col, 256)
        both = mm(left_side[pl.ds(slot * 2 * flat, 2 * flat), :], f_hi[:, cols])
        low = mm(left_side[pl.ds(slot * 2 * flat, flat), :], f_lo[:, cols])
        return both[:flat] + both[flat:] + low

    def column(i):
        target = lax.rem(my_z + 1 + i, 4)
        return target, pl.multiple_of(target * 256, 256)

    def fwd_copy(spec, got, kind, dest, at, count):
        return pltpu.make_async_remote_copy(
            src_ref=spec.at[pl.ds(at, count), :, own_cols(dest)],
            dst_ref=got.at[pl.ds(at, count), own_rows(me), :],
            send_sem=fwd_send.at[kind, dest],
            recv_sem=fwd_recv.at[kind, me],
            device_id={"gx": gx, "yz": dest},
            device_id_type=MESH,
        )

    def fwd_own(spec, got, kind, at, count):
        return pltpu.make_async_copy(
            spec.at[pl.ds(at, count), :, own_cols(me)],
            got.at[pl.ds(at, count), own_rows(me), :],
            fwd_recv.at[kind, me],
        )

    def fwd_wait(spec, got, kind, at, count):
        fwd_own(spec, got, kind, at, count).wait()

        def step(d, carry):
            src = peer(d)
            where = got.at[pl.ds(at, count), own_rows(src), :]
            pltpu.make_async_remote_copy(
                src_ref=where, dst_ref=where, send_sem=fwd_send.at[kind, src],
                recv_sem=fwd_recv.at[kind, src], device_id={"gx": gx, "yz": src},
                device_id_type=MESH,
            ).wait_recv()
            return carry

        lax.fori_loop(1, GROUPS, step, 0)

    def send_column(spec, got, kind, i, at, count):
        target, _ = column(i)
        for side in range(2):
            dest = target * 2 + side

            @pl.when(dest != me)
            def _():
                fwd_copy(spec, got, kind, dest, at, count).start()

    def put_u(c, p, at):
        store_split(at, ghost[c, pl.ds(3 + p, 2)].reshape(48, width))

    def modes_of(spec, i, make):
        _, col = column(i)
        if make:
            build(col)
        spec[:, :, pl.ds(col, 256)] = to_modes(0, col).reshape(18, rows, 256)

    loads[1].wait()
    loads[2].wait()
    loads[0].wait()
    pairs_loop(put_u)
    modes_of(spec_u, 0, True)
    loads[3].wait()
    pl.semaphore_wait(barrier, GROUPS + 1)
    vel_halo = halo(ghost, 3, 0, True)
    guess_halo = halo(guess, 2, 2, False)
    for copy in vel_halo + guess_halo:
        copy.start()
    send_column(spec_u, got_u, 0, 0, 0, 18)

    def rest_u(i, carry):
        modes_of(spec_u, i, True)
        send_column(spec_u, got_u, 0, i, 0, 18)
        return carry

    lax.fori_loop(1, 4, rest_u, 0)
    fwd_own(spec_u, got_u, 0, 0, 18).start()

    def put_c(c, p, at):
        u_z = ghost[2, pl.ds(3 + p, 2)]
        store_split(at, (-u_z * ghost[c, pl.ds(3 + p, 2)]).reshape(48, width))

    pairs_loop(put_c)

    def all_c(i, carry):
        modes_of(spec_c, i, False)
        send_column(spec_c, got_c, 1, i, 0, 18)
        return carry

    lax.fori_loop(0, 4, all_c, 0)
    fwd_own(spec_c, got_c, 1, 0, 18).start()

    for copy in vel_halo:
        copy.wait_recv()
    shift = shift_ref[0]

    def fix(start, amount, extra):
        def step(i, carry):
            c, p = i // 3, lax.rem(i, 3) + start
            once = pltpu.roll(ghost[c, p], amount, 1)
            ghost[c, p] = (1.0 - fraction) * once + fraction * pltpu.roll(once, extra, 1)
            return carry

        lax.fori_loop(0, 9, step, 0)

    @pl.when(gx == 0)
    def _():
        fix(0, lax.rem(width - shift, width), width - 1)

    @pl.when(gx == slabs - 1)
    def _():
        fix(planes + 3, shift, 1)

    total_x = planes * slabs
    omega = 2.0 / total_x

    def put_ab(i, carry):
        c, p = i // 3, lax.rem(i, 3) * 2
        terms_a = []
        terms_b = []
        for q in range(2):
            at = p + q + 3
            u_x = [ghost[0, at + o] for o in range(-3, 4)]
            u_i = [ghost[c, at + o] for o in range(-3, 4)]
            prod = [x * y for x, y in zip(u_x, u_i)]
            slope = (
                (45.0 / 60.0) * (prod[4] - prod[2])
                - (9.0 / 60.0) * (prod[5] - prod[1])
                + (1.0 / 60.0) * (prod[6] - prod[0])
            )
            bend = (
                (2.0 / 180.0) * (u_i[6] + u_i[0])
                - (27.0 / 180.0) * (u_i[5] + u_i[1])
                + (270.0 / 180.0) * (u_i[4] + u_i[2])
                - (490.0 / 180.0) * u_i[3]
            )
            u_y = ghost[1, at]
            weight_y = jnp.where(c == 0, 2.0 * omega, 0.0).astype(F32)
            weight_x = jnp.where(c == 1, -(2.0 - shear_param) * omega, 0.0).astype(F32)
            terms_a.append(viscosity * bend - slope + (weight_y * u_y + weight_x * u_x[3]))
            place = (gx * planes + p + q).astype(F32) + 0.5 - total_x / 2.0
            background = -shear_param * omega * place
            terms_b.append(-(u_y + background) * u_i[3])
        store_split(i * 48, jnp.concatenate(terms_a, axis=0))
        store_split(2 * flat + i * 48, jnp.concatenate(terms_b, axis=0))
        return carry

    lax.fori_loop(0, 9, put_ab, 0)
    loads[4].wait()

    def combine(i, carry):
        _, col = column(i)
        ya = to_modes(0, col)
        yb = to_modes(1, col)
        for side in range(2):
            wide = pl.ds(pl.multiple_of(col + side * lanes, lanes), lanes)
            cut = slice(side * lanes, (side + 1) * lanes)
            ky = wavey[0:1, wide]
            yu = spec_u[:, :, wide].reshape(flat, lanes)
            out = ya[:, cut] + turned(yb[:, cut]) * ky - (viscosity * ky * ky) * yu
            spec_w[:, :, wide] = out.reshape(18, rows, lanes)
        return carry

    lax.fori_loop(0, 4, combine, 0)
    w_parts = ((2, 0, 6), (3, 6, 6), (4, 12, 2), (5, 14, 2), (6, 16, 2))
    for kind, at, count in w_parts:
        def send_w(i, carry, kind=kind, at=at, count=count):
            send_column(spec_w, got_w, kind, i, at, count)
            return carry

        lax.fori_loop(0, 4, send_w, 0)
        fwd_own(spec_w, got_w, kind, at, count).start()

    for i in (5, 6, 7, 8, 9):
        loads[i].wait()
    own_ky = wavey[0:1, own_cols(me)]
    recip[...] = 1.0 / (2.0 + own_ky * own_ky + wavez[...] * wavez[...])

    def build_back(g, carry):
        cosine = icoarse[pl.ds(g, 1), :]
        sine = icoarse[pl.ds(g + GROUPS, 1), :]
        for part in range(2):
            if part == 0:
                value = cosine * ifine[0] + sine * ifine[1]
            else:
                value = cosine * ifine[1] - sine * ifine[0]
            high, low = split(value)
            where = pl.ds(pl.multiple_of(g * lanes + part * half, half), half)
            f_hi[where, :] = high
            f_lo[where, :] = low
        return carry

    lax.fori_loop(0, GROUPS, build_back, 0)
    top = lax.broadcasted_iota(jnp.int32, (16, width), 0) == 0
    for table in (f_hi, f_lo):
        lines = table[0:16, :].astype(F32)
        table[0:16, :] = jnp.where(top, lines * 0.5, lines).astype(BF16)

    cosine = edge[0:1, :]
    sine = edge[1:2, :]

    def rotate_ends(lower, upper):
        @pl.when(gx == 0)
        def _():
            for ref, j in lower:
                value = ref[j]
                ref[j] = value * cosine + turned(value) * sine

        @pl.when(gx == slabs - 1)
        def _():
            for ref, j in upper:
                value = ref[j]
                ref[j] = value * cosine - turned(value) * sine

    for copy in guess_halo:
        copy.wait_recv()
    rotate_ends(((guess, 0), (guess, 1)), ((guess, 8), (guess, 9)))

    def z_pair(ref, at, kind):
        value = jnp.concatenate([ref[at], ref[at + 1]], axis=1)
        high, low = split(value)
        return mm(zmat[kind], high), mm(zmat[kind, pl.ds(0, 2 * depth)], low)

    def z_join(parts):
        total = sum(wide[: 2 * depth] + wide[2 * depth :] + low for wide, low in parts)
        out = []
        for q in range(2):
            cut = slice(q * lanes, (q + 1) * lanes)
            out.append(total[:depth, cut] + turned(total[depth:, cut]))
        return out

    fwd_wait(spec_u, got_u, 0, 0, 18)
    fwd_wait(spec_c, got_c, 1, 0, 18)

    def z_first(i, carry):
        at = i * 2
        values = z_join([z_pair(got_c, at, 1), z_pair(got_u, at, 2)])
        tend[at] = values[0]
        tend[at + 1] = values[1]
        return carry

    lax.fori_loop(0, 9, z_first, 0)

    def z_last(c, pair):
        at = c * planes + pair * 2
        values = z_join([z_pair(got_w, at, 0)])
        for q in range(2):
            value = tend[at + q] + values[q]
            tend[at + q] = value
            values[q] = value
        return values

    fwd_wait(spec_w, got_w, 2, 0, 6)

    def last_x(pair, carry):
        values = z_last(0, pair)
        for q in range(2):
            tend_x[2 * pair + q + 1] = values[q]
        return carry

    lax.fori_loop(0, 3, last_x, 0)
    x_halo = halo(tend_x, 1, 4, False)
    for copy in x_halo:
        copy.start()

    fwd_wait(spec_w, got_w, 3, 6, 6)

    def last_y(pair, carry):
        values = z_last(1, pair)
        for q in range(2):
            cross[2 * pair + q] = turned(values[q]) * own_ky
        return carry

    lax.fori_loop(0, 3, last_y, 0)

    def last_z(pair, carry):
        fwd_wait(spec_w, got_w, 4 + pair, 12 + 2 * pair, 2)
        values = z_last(2, pair)
        for q in range(2):
            j = 2 * pair + q
            cross[j] = cross[j] + turned(values[q]) * wavez[...]
        return carry

    lax.fori_loop(0, 3, last_z, 0)

    def sweep_own(j):
        diverge[j + 1] = 0.5 * (tend_x[j + 2] - tend_x[j]) + cross[j]
        first[j + 1] = (guess[j + 3] + guess[j + 1] - diverge[j + 1]) * recip[...]

    for j in (1, 4):
        sweep_own(j)
    late[0] = 0.5 * tend_x[2] + cross[0]
    late[1] = first[2]
    late[2] = 0.5 * tend_x[5] - cross[5]
    late[3] = first[5]
    late_halo = (
        x_copy(late.at[pl.ds(0, 2)], late.at[pl.ds(6, 2)], 6, left),
        x_copy(late.at[pl.ds(2, 2)], late.at[pl.ds(4, 2)], 7, right),
    )
    for copy in late_halo:
        copy.start()
    for copy in x_halo:
        copy.wait_recv()
    rotate_ends(((tend_x, 0),), ((tend_x, planes + 1),))
    for j in (0, 2, 3, 5):
        sweep_own(j)

    def sweep_again(j):
        press[j + 1] = (first[j + 2] + first[j] - diverge[j + 1]) * recip[...]

    for j in (1, 2, 3, 4):
        sweep_again(j)
    loads[10].wait()

    def inv_copy(pair, c, dest):
        at = pair * 6 + c * 2
        return pltpu.make_async_remote_copy(
            src_ref=spatial.at[pl.ds(at, 2), own_rows(dest), :],
            dst_ref=got_s.at[pl.ds(at, 2), :, own_cols(me)],
            send_sem=inv_send.at[pair * 3 + c, dest],
            recv_sem=inv_recv.at[pair * 3 + c, me],
            device_id={"gx": gx, "yz": dest},
            device_id_type=MESH,
        )

    def inv_own(pair, c):
        at = pair * 6 + c * 2
        return pltpu.make_async_copy(
            spatial.at[pl.ds(at, 2), own_rows(me), :],
            got_s.at[pl.ds(at, 2), :, own_cols(me)],
            inv_recv.at[pair * 3 + c, me],
        )

    def finish(pair):
        for q in range(2):
            p = 2 * pair + q
            here = press[p + 1]
            side = turned(here)
            pout[p] = here
            slopes = (0.5 * (press[p + 2] - press[p]), side * own_ky, side * wavez[...])
            for c in range(3):
                qnext[c, p] = keep_weight * qold[c, p] + time_step * (
                    tend[c * planes + p] - slopes[c]
                )

        def back(c, carry):
            at = pair * 6 + c * 2
            values = z_join([z_pair(qnext.at[c], 2 * pair, 3)])
            spatial[at] = values[0]
            spatial[at + 1] = values[1]

            def send(d, inner):
                inv_copy(pair, c, peer(d)).start()
                return inner

            lax.fori_loop(1, GROUPS, send, 0)
            inv_own(pair, c).start()
            return carry

        lax.fori_loop(0, 3, back, 0)

    finish(1)
    for copy in late_halo:
        copy.wait_recv()
    rotate_ends(((late, 4), (late, 5)), ((late, 6), (late, 7)))
    low = 0.5 * tend_x[1] - late[4]
    first[0] = (guess[2] + guess[0] - low) * recip[...]
    press[0] = (first[1] + late[5] - low) * recip[...]
    high = late[6] - 0.5 * tend_x[6]
    first[7] = (guess[9] + guess[7] - high) * recip[...]
    press[7] = (late[7] + first[6] - high) * recip[...]
    for j in (0, 5):
        sweep_again(j)

    def finish_ends(i, carry):
        finish(i * 2)
        return carry

    lax.fori_loop(0, 2, finish_ends, 0)

    rows_c = planes * rows

    def arrive(i, carry):
        pair = jnp.where(i == 0, 1, jnp.where(i == 1, 0, 2))
        for c in range(3):
            inv_own(pair, c).wait()

            def step(d, inner, c=c):
                src = peer(d)
                where = got_s.at[pl.ds(pair * 6 + c * 2, 2), :, own_cols(src)]
                pltpu.make_async_remote_copy(
                    src_ref=where, dst_ref=where, send_sem=inv_send.at[pair * 3 + c, src],
                    recv_sem=inv_recv.at[pair * 3 + c, src], device_id={"gx": gx, "yz": src},
                    device_id_type=MESH,
                ).wait_recv()
                return inner

            lax.fori_loop(1, GROUPS, step, 0)
        high, low = split(got_s[pl.ds(pair * 6, 6)].reshape(rows_c, width))
        left_side[0:rows_c, :] = high
        left_side[rows_c : 2 * rows_c, :] = low

        def cells(k, inner):
            cols = pl.ds(pl.multiple_of(k * 256, 256), 256)
            both = mm(left_side[0 : 2 * rows_c, :], f_hi[:, cols])
            out = both[:rows_c] + both[rows_c:] + mm(left_side[0:rows_c, :], f_lo[:, cols])
            for c in range(3):
                for q in range(2):
                    at = (c * 2 + q) * rows
                    p = 2 * pair + q
                    vnext[c, p, :, cols] = ghost[c, p + 3, :, cols] + out[at : at + rows]
            return inner

        lax.fori_loop(0, 4, cells, 0)
        return carry

    lax.fori_loop(0, 3, arrive, 0)

    def drain(d, carry):
        dest = peer(d)
        fwd_copy(spec_u, got_u, 0, dest, 0, 18).wait_send()
        fwd_copy(spec_c, got_c, 1, dest, 0, 18).wait_send()
        for kind, at, count in w_parts:
            fwd_copy(spec_w, got_w, kind, dest, at, count).wait_send()
        for pair in range(3):
            for c in range(3):
                inv_copy(pair, c, dest).wait_send()
        return carry

    lax.fori_loop(1, GROUPS, drain, 0)
    for copy in vel_halo + guess_halo + x_halo + late_halo:
        copy.wait_send()


def local(slabs, vel, q_old, pressure_guess, shear_shift):
    width = vel.shape[3]
    depth = q_old.shape[2]
    half = width // (2 * GROUPS)
    planes, rows = vel.shape[1], vel.shape[2]
    consts = tables(width, depth)
    modes = lax.axis_index("yz") * half + jnp.arange(2 * half, dtype=jnp.int32) % half
    angle = (2.0 * math.pi / width) * (
        (modes * shear_shift[0] % width).astype(F32) + fraction * modes.astype(F32)
    )
    edge = jnp.stack([jnp.cos(angle), jnp.sin(angle)])
    any_spec = pl.BlockSpec(memory_space=pl.ANY)
    vmem = lambda *shape: pltpu.VMEM(shape, F32)
    wide = lambda n: pltpu.VMEM((n, depth, 2 * half), F32)
    flat = 3 * planes * rows
    scratch = [
        vmem(3, planes + 6, rows, width),
        vmem(*consts[0].shape),
        vmem(2, *consts[1].shape),
        vmem(*consts[2].shape),
        vmem(*consts[3].shape),
        vmem(*consts[4].shape),
        vmem(*consts[5].shape),
        pltpu.VMEM(consts[6].shape, BF16),
        vmem(2, 2 * half),
        vmem(3, planes, depth, 2 * half),
        pltpu.VMEM((width, width), BF16),
        pltpu.VMEM((width, width), BF16),
        pltpu.VMEM((4 * flat, width), BF16),
        vmem(3 * planes, rows, width),
        vmem(3 * planes, rows, width),
        vmem(3 * planes, rows, width),
        wide(3 * planes),
        wide(3 * planes),
        wide(3 * planes),
        wide(3 * planes),
        wide(planes + 2),
        wide(planes),
        wide(planes + 4),
        wide(8),
        vmem(depth, 2 * half),
        wide(planes + 2),
        wide(planes + 2),
        wide(planes + 2),
        wide(3 * planes),
        vmem(3 * planes, rows, width),
        pltpu.SemaphoreType.DMA((11,)),
        pltpu.SemaphoreType.DMA((8,)),
        pltpu.SemaphoreType.DMA((8,)),
        pltpu.SemaphoreType.DMA((7, GROUPS)),
        pltpu.SemaphoreType.DMA((7, GROUPS)),
        pltpu.SemaphoreType.DMA((9, GROUPS)),
        pltpu.SemaphoreType.DMA((9, GROUPS)),
    ]
    call = pl.pallas_call(
        functools.partial(body, slabs),
        out_shape=(
            jax.ShapeDtypeStruct(vel.shape, F32),
            jax.ShapeDtypeStruct(q_old.shape, F32),
            jax.ShapeDtypeStruct(pressure_guess.shape, F32),
        ),
        in_specs=[pl.BlockSpec(memory_space=pltpu.SMEM)] + [any_spec] * 11,
        out_specs=(pl.BlockSpec(memory_space=pltpu.VMEM),) * 3,
        scratch_shapes=scratch,
        compiler_params=pltpu.CompilerParams(
            collective_id=0, has_side_effects=True, vmem_limit_bytes=48 * 2**20
        ),
        name="section",
    )
    return call(shear_shift, vel, q_old, pressure_guess, edge, *consts)


def solution(mesh):
    in_specs = (P(None, "gx", "yz", None), P(None, "gx", None, "yz"), P("gx", None, "yz"), P())
    out_specs = (P(None, "gx", "yz", None), P(None, "gx", None, "yz"), P("gx", None, "yz"))
    return jax.shard_map(
        functools.partial(local, mesh.shape["gx"]),
        mesh=mesh, in_specs=in_specs, out_specs=out_specs, check_vma=False,
    )
```

```python
import functools
import math

import jax
import jax.numpy as jnp
import numpy as np
from jax import lax
from jax.experimental import pallas as pl
from jax.experimental.pallas import tpu as pltpu
from jax.sharding import PartitionSpec as P

viscosity = 0.05
time_step = 0.2
keep_weight = -5.0 / 9.0
section_weight = 15.0 / 16.0
shear_param = 1.5
fraction = 0.375
GROUPS = 8
MESH = pl.DeviceIdType.MESH
F32 = jnp.float32
BF16 = jnp.bfloat16


def tables(width_y, depth_z):
    half = width_y // (2 * GROUPS)
    lanes = np.arange(width_y)
    mode = lanes // (2 * half) * half + lanes % half
    is_im = (lanes // half) % 2 == 1
    coarse = np.arange(width_y // half)
    fine = np.arange(half)

    def angle(n, k):
        return 2.0 * np.pi / width_y * ((n[:, None] * k[None, :]) % width_y)

    scale = 1.0 / math.sqrt(width_y)
    alpha = angle(coarse * half, mode)
    beta = angle(fine, mode)
    fwd_coarse = np.concatenate([np.cos(alpha), np.sin(alpha)])
    fwd_fine = scale * np.where(is_im[None], -np.sin(beta), np.cos(beta))
    cells = np.arange(width_y)
    alpha = angle(np.arange(GROUPS) * half, cells)
    beta = angle(fine, cells)
    inv_coarse = np.concatenate([np.cos(alpha), np.sin(alpha)])
    inv_fine = (2.0 * section_weight * scale) * np.stack([np.cos(beta), -np.sin(beta)])
    wave_y = 2.0 * np.pi / width_y * mode[None, :]
    m = np.arange(depth_z)
    signed = np.where(m < depth_z // 2, m, m - depth_z)
    wave_z = (2.0 * np.pi / depth_z * signed)[:, None]
    angle_z = 2.0 * np.pi / depth_z * ((m[:, None] * m[None, :]) % depth_z)
    forward = np.exp(-1j * angle_z) / math.sqrt(depth_z)
    mats = [
        forward,
        1j * wave_z * forward,
        -viscosity * wave_z * wave_z * forward,
        np.exp(1j * angle_z) / math.sqrt(depth_z),
    ]
    stacked = []
    for mat in mats:
        both = np.concatenate([mat.real, mat.imag]).astype(np.float32)
        high = both.astype(BF16)
        low = (both - high.astype(np.float32)).astype(BF16)
        stacked.append(np.concatenate([high, low]))
    as32 = lambda v: jnp.asarray(np.asarray(v, np.float32))
    return (
        as32(fwd_coarse),
        as32(fwd_fine),
        as32(inv_coarse),
        as32(inv_fine),
        as32(wave_y),
        as32(np.broadcast_to(wave_z, (depth_z, 2 * half))),
        jnp.asarray(np.stack(stacked)),
    )


def split(value):
    high = value.astype(BF16)
    low = (value - high.astype(F32)).astype(BF16)
    return high, low


def mm(a, b):
    return jnp.dot(a, b, preferred_element_type=F32)


def body(
    slabs,
    shift_ref,
    vel_hbm,
    qold_hbm,
    guess_hbm,
    edge_hbm,
    fcoarse_hbm,
    ffine_hbm,
    icoarse_hbm,
    ifine_hbm,
    wavey_hbm,
    wavez_hbm,
    zmat_hbm,
    vnext_hbm,
    qnext_hbm,
    pout_hbm,
    ghost,
    relay,
    fcoarse,
    ffine,
    icoarse,
    ifine,
    wavey,
    wavez,
    zmat,
    edge,
    qold,
    f_hi,
    f_lo,
    left_side,
    spec_u,
    spec_c,
    spec_w,
    got_u,
    got_c,
    got_w,
    tend,
    tend_x,
    cross,
    guess,
    late,
    recip,
    diverge,
    first,
    press,
    spatial,
    got_s,
    load_sem,
    halo_send,
    halo_recv,
    fwd_send,
    fwd_recv,
    inv_send,
    inv_recv,
    out_sem,
):
    gx = lax.axis_index("gx")
    me = lax.axis_index("yz")
    my_z = me // 2
    right = lax.rem(gx + 1, slabs)
    left = lax.rem(gx + slabs - 1, slabs)
    relayed = slabs == 16
    near = 384
    planes = 6
    rows = 24
    width = 1024
    depth = 192
    lanes = 128
    half = 64
    flat = planes * rows * 3

    def peer(d):
        return lax.rem(me + d, GROUPS)

    def own_cols(ref_index):
        return pl.ds(pl.multiple_of(ref_index * lanes, lanes), lanes)

    def own_rows(ref_index):
        return pl.ds(pl.multiple_of(ref_index * rows, 8), rows)

    loads = [
        (vel_hbm, ghost.at[:, pl.ds(3, planes)]),
        (fcoarse_hbm, fcoarse),
        (ffine_hbm, ffine.at[0]),
        (guess_hbm, guess.at[pl.ds(2, planes)]),
        (wavey_hbm, wavey),
        (edge_hbm, edge),
        (zmat_hbm, zmat),
        (wavez_hbm, wavez),
        (icoarse_hbm, icoarse),
        (ifine_hbm, ifine),
        (qold_hbm, qold),
    ]
    loads = [pltpu.make_async_copy(s, d, load_sem.at[i]) for i, (s, d) in enumerate(loads)]
    for i in (1, 2, 0, 3, 4, 5, 6, 7, 8, 9, 10):
        loads[i].start()

    barrier = pltpu.get_barrier_semaphore()
    for d in range(1, GROUPS):
        pl.semaphore_signal(
            barrier, inc=1, device_id={"gx": gx, "yz": peer(d)}, device_id_type=MESH
        )
    for side in (left, right):
        pl.semaphore_signal(barrier, inc=1, device_id={"gx": side, "yz": me}, device_id_type=MESH)
    place = lax.rem(gx, 8)
    ends_right = place == 7
    ends_left = place == 0
    helps_left = place == 3
    helps_right = place == 4
    helper = ends_right | ends_left | helps_left | helps_right
    far_side = lax.rem(gx + jnp.where(ends_right | helps_left, 5, slabs - 5), slabs)
    near_side = lax.rem(gx + jnp.where(ends_right | helps_right, slabs - 4, 4), slabs)
    if relayed:

        @pl.when(helper)
        def _():
            for side in (far_side, near_side):
                pl.semaphore_signal(
                    barrier, inc=1, device_id={"gx": side, "yz": me}, device_id_type=MESH
                )

    def x_copy(src, dst, slot, target):
        return pltpu.make_async_remote_copy(
            src_ref=src, dst_ref=dst, send_sem=halo_send.at[slot], recv_sem=halo_recv.at[slot],
            device_id={"gx": target, "yz": me}, device_id_type=MESH,
        )

    def halo(ref, count, slot, lead):
        def at(start):
            return ref.at[:, pl.ds(start, count)] if lead else ref.at[pl.ds(start, count)]

        return (
            x_copy(at(count), at(count + planes), slot, left),
            x_copy(at(planes), at(0), slot + 1, right),
        )

    sign = jnp.where(lax.broadcasted_iota(jnp.int32, (1, lanes), 1) < half, -1.0, 1.0).astype(F32)

    def turned(value):
        return pltpu.roll(value, half, 1) * sign

    def store_split(at, value, gap=flat):
        high, low = split(value)
        left_side[pl.ds(pl.multiple_of(at, 48), 48), :] = high
        left_side[pl.ds(pl.multiple_of(at + gap, 48), 48), :] = low

    def build(col):
        cols = pl.ds(col, 256)
        for side in range(2):
            part = pl.ds(pl.multiple_of(col + side * lanes, lanes), lanes)
            ffine[1, :, part] = -turned(ffine[0, :, part])

        def step(a, carry):
            value = (
                fcoarse[pl.ds(a, 1), cols] * ffine[0, :, cols]
                + fcoarse[pl.ds(a + width // half, 1), cols] * ffine[1, :, cols]
            )
            high, low = split(value)
            where = pl.ds(pl.multiple_of(a * half, half), half)
            f_hi[where, cols] = high
            f_lo[where, cols] = low
            return carry

        lax.fori_loop(0, width // half, step, 0)

    def pairs_loop(write):
        def step(i, carry):
            write(i // 3, lax.rem(i, 3) * 2, i * 48)
            return carry

        lax.fori_loop(0, 9, step, 0)

    def to_modes(slot, col):
        cols = pl.ds(col, 256)
        both = mm(left_side[pl.ds(slot * 2 * flat, 2 * flat), :], f_hi[:, cols])
        low = mm(left_side[pl.ds(slot * 2 * flat, flat), :], f_lo[:, cols])
        return both[:flat] + both[flat:] + low

    def column(i):
        target = lax.rem(my_z + 1 + i, 4)
        return target, pl.multiple_of(target * 256, 256)

    def fwd_copy(spec, got, kind, dest, at, count):
        return pltpu.make_async_remote_copy(
            src_ref=spec.at[pl.ds(at, count), :, own_cols(dest)],
            dst_ref=got.at[pl.ds(at, count), own_rows(me), :],
            send_sem=fwd_send.at[kind, dest],
            recv_sem=fwd_recv.at[kind, me],
            device_id={"gx": gx, "yz": dest},
            device_id_type=MESH,
        )

    def fwd_own(spec, got, kind, at, count):
        return pltpu.make_async_copy(
            spec.at[pl.ds(at, count), :, own_cols(me)],
            got.at[pl.ds(at, count), own_rows(me), :],
            fwd_recv.at[kind, me],
        )

    def fwd_wait(spec, got, kind, at, count):
        fwd_own(spec, got, kind, at, count).wait()

        def step(d, carry):
            src = peer(d)
            where = got.at[pl.ds(at, count), own_rows(src), :]
            pltpu.make_async_remote_copy(
                src_ref=where, dst_ref=where, send_sem=fwd_send.at[kind, src],
                recv_sem=fwd_recv.at[kind, src], device_id={"gx": gx, "yz": src},
                device_id_type=MESH,
            ).wait_recv()
            return carry

        lax.fori_loop(1, GROUPS, step, 0)

    def send_column(spec, got, kind, i, at, count):
        target, _ = column(i)
        for side in range(2):
            dest = target * 2 + side

            @pl.when(dest != me)
            def _():
                fwd_copy(spec, got, kind, dest, at, count).start()

    def put_u(c, p, at):
        store_split(at, ghost[c, pl.ds(3 + p, 2)].reshape(48, width))

    def modes_of(spec, i, make):
        _, col = column(i)
        if make:
            build(col)
        spec[:, :, pl.ds(col, 256)] = to_modes(0, col).reshape(18, rows, 256)

    loads[1].wait()
    loads[2].wait()
    loads[0].wait()
    pairs_loop(put_u)
    modes_of(spec_u, 0, True)
    loads[3].wait()
    vel_halo = halo(ghost, 3, 0, True)
    guess_halo = halo(guess, 2, 2, False)

    def part(ref, start, side):
        cols = pl.ds(0, near) if side == 0 else pl.ds(near, width - near)
        return ref.at[:, pl.ds(start, 3), :, cols]

    near_halo = (
        x_copy(part(ghost, 3, 0), part(ghost, planes + 3, 0), 0, left),
        x_copy(part(ghost, planes, 0), part(ghost, 0, 0), 1, right),
    )
    to_relay = (
        x_copy(part(ghost, 3, 1), relay, 8, far_side),
        x_copy(part(ghost, planes, 1), relay, 8, far_side),
    )
    from_relay = (
        x_copy(relay, part(ghost, planes + 3, 1), 9, near_side),
        x_copy(relay, part(ghost, 0, 1), 9, near_side),
    )

    if relayed:
        pl.semaphore_wait(barrier, jnp.where(helper, GROUPS + 3, GROUPS + 1))
        for i, ends in ((0, ends_left), (1, ends_right)):

            @pl.when(ends)
            def _():
                to_relay[i].start()
                near_halo[i].start()

            @pl.when(jnp.logical_not(ends))
            def _():
                vel_halo[i].start()

    else:
        pl.semaphore_wait(barrier, GROUPS + 1)
        for copy in vel_halo:
            copy.start()
    for copy in guess_halo:
        copy.start()
    send_column(spec_u, got_u, 0, 0, 0, 18)

    def rest_u(i, carry):
        modes_of(spec_u, i, True)
        send_column(spec_u, got_u, 0, i, 0, 18)
        return carry

    lax.fori_loop(1, 4, rest_u, 0)
    fwd_own(spec_u, got_u, 0, 0, 18).start()

    def put_c(c, p, at):
        u_z = ghost[2, pl.ds(3 + p, 2)]
        store_split(at, (-u_z * ghost[c, pl.ds(3 + p, 2)]).reshape(48, width))

    pairs_loop(put_c)

    def all_c(i, carry):
        modes_of(spec_c, i, False)
        send_column(spec_c, got_c, 1, i, 0, 18)
        return carry

    lax.fori_loop(0, 4, all_c, 0)
    fwd_own(spec_c, got_c, 1, 0, 18).start()

    if relayed:
        for i, helps in ((0, helps_left), (1, helps_right)):

            @pl.when(helps)
            def _():
                to_relay[i].wait_recv()
                from_relay[i].start()

        for i, ends in ((0, ends_right), (1, ends_left)):

            @pl.when(ends)
            def _():
                near_halo[i].wait_recv()
                from_relay[i].wait_recv()

            @pl.when(jnp.logical_not(ends))
            def _():
                vel_halo[i].wait_recv()

    else:
        for copy in vel_halo:
            copy.wait_recv()
    shift = shift_ref[0]

    def fix(start, amount, extra):
        def step(i, carry):
            c, p = i // 3, lax.rem(i, 3) + start
            once = pltpu.roll(ghost[c, p], amount, 1)
            ghost[c, p] = (1.0 - fraction) * once + fraction * pltpu.roll(once, extra, 1)
            return carry

        lax.fori_loop(0, 9, step, 0)

    @pl.when(gx == 0)
    def _():
        fix(0, lax.rem(width - shift, width), width - 1)

    @pl.when(gx == slabs - 1)
    def _():
        fix(planes + 3, shift, 1)

    total_x = planes * slabs
    omega = 2.0 / total_x

    def put_ab(i, carry):
        c, p = i // 3, lax.rem(i, 3) * 2
        terms_a = []
        terms_b = []
        for q in range(2):
            at = p + q + 3
            u_x = [ghost[0, at + o] for o in range(-3, 4)]
            u_i = [ghost[c, at + o] for o in range(-3, 4)]
            prod = [x * y for x, y in zip(u_x, u_i)]
            slope = (
                (45.0 / 60.0) * (prod[4] - prod[2])
                - (9.0 / 60.0) * (prod[5] - prod[1])
                + (1.0 / 60.0) * (prod[6] - prod[0])
            )
            bend = (
                (2.0 / 180.0) * (u_i[6] + u_i[0])
                - (27.0 / 180.0) * (u_i[5] + u_i[1])
                + (270.0 / 180.0) * (u_i[4] + u_i[2])
                - (490.0 / 180.0) * u_i[3]
            )
            u_y = ghost[1, at]
            weight_y = jnp.where(c == 0, 2.0 * omega, 0.0).astype(F32)
            weight_x = jnp.where(c == 1, -(2.0 - shear_param) * omega, 0.0).astype(F32)
            terms_a.append(viscosity * bend - slope + (weight_y * u_y + weight_x * u_x[3]))
            place = (gx * planes + p + q).astype(F32) + 0.5 - total_x / 2.0
            background = -shear_param * omega * place
            terms_b.append(-(u_y + background) * u_i[3])
        store_split(i * 48, jnp.concatenate(terms_a, axis=0))
        store_split(2 * flat + i * 48, jnp.concatenate(terms_b, axis=0))
        return carry

    lax.fori_loop(0, 9, put_ab, 0)
    loads[4].wait()

    def combine(i, carry):
        _, col = column(i)
        ya = to_modes(0, col)
        yb = to_modes(1, col)
        for side in range(2):
            wide = pl.ds(pl.multiple_of(col + side * lanes, lanes), lanes)
            cut = slice(side * lanes, (side + 1) * lanes)
            ky = wavey[0:1, wide]
            yu = spec_u[:, :, wide].reshape(flat, lanes)
            out = ya[:, cut] + turned(yb[:, cut]) * ky - (viscosity * ky * ky) * yu
            spec_w[:, :, wide] = out.reshape(18, rows, lanes)
        return carry

    lax.fori_loop(0, 4, combine, 0)
    w_parts = ((2, 0, 6), (3, 6, 6), (4, 12, 2), (5, 14, 2), (6, 16, 2))
    for kind, at, count in w_parts:
        def send_w(i, carry, kind=kind, at=at, count=count):
            send_column(spec_w, got_w, kind, i, at, count)
            return carry

        lax.fori_loop(0, 4, send_w, 0)
        fwd_own(spec_w, got_w, kind, at, count).start()

    for i in (5, 6, 7, 8, 9):
        loads[i].wait()
    own_ky = wavey[0:1, own_cols(me)]
    recip[...] = 1.0 / (2.0 + own_ky * own_ky + wavez[...] * wavez[...])

    def build_back(g, carry):
        cosine = icoarse[pl.ds(g, 1), :]
        sine = icoarse[pl.ds(g + GROUPS, 1), :]
        for part in range(2):
            if part == 0:
                value = cosine * ifine[0] + sine * ifine[1]
            else:
                value = cosine * ifine[1] - sine * ifine[0]
            high, low = split(value)
            where = pl.ds(pl.multiple_of(g * lanes + part * half, half), half)
            f_hi[where, :] = high
            f_lo[where, :] = low
        return carry

    lax.fori_loop(0, GROUPS, build_back, 0)
    top = lax.broadcasted_iota(jnp.int32, (16, width), 0) == 0
    for table in (f_hi, f_lo):
        lines = table[0:16, :].astype(F32)
        table[0:16, :] = jnp.where(top, lines * 0.5, lines).astype(BF16)

    cosine = edge[0:1, :]
    sine = edge[1:2, :]

    def rotate_ends(lower, upper):
        @pl.when(gx == 0)
        def _():
            for ref, j in lower:
                value = ref[j]
                ref[j] = value * cosine + turned(value) * sine

        @pl.when(gx == slabs - 1)
        def _():
            for ref, j in upper:
                value = ref[j]
                ref[j] = value * cosine - turned(value) * sine

    for copy in guess_halo:
        copy.wait_recv()
    rotate_ends(((guess, 0), (guess, 1)), ((guess, 8), (guess, 9)))

    def z_pair(ref, at, kind):
        value = jnp.concatenate([ref[at], ref[at + 1]], axis=1)
        high, low = split(value)
        return mm(zmat[kind], high), mm(zmat[kind, pl.ds(0, 2 * depth)], low)

    def z_join(parts):
        total = sum(wide[: 2 * depth] + wide[2 * depth :] + low for wide, low in parts)
        out = []
        for q in range(2):
            cut = slice(q * lanes, (q + 1) * lanes)
            out.append(total[:depth, cut] + turned(total[depth:, cut]))
        return out

    fwd_wait(spec_u, got_u, 0, 0, 18)
    fwd_wait(spec_c, got_c, 1, 0, 18)

    def z_first(i, carry):
        at = i * 2
        values = z_join([z_pair(got_c, at, 1), z_pair(got_u, at, 2)])
        tend[at] = values[0]
        tend[at + 1] = values[1]
        return carry

    lax.fori_loop(0, 9, z_first, 0)

    def z_last(c, pair):
        at = c * planes + pair * 2
        values = z_join([z_pair(got_w, at, 0)])
        for q in range(2):
            value = tend[at + q] + values[q]
            tend[at + q] = value
            values[q] = value
        return values

    fwd_wait(spec_w, got_w, 2, 0, 6)

    def last_x(pair, carry):
        values = z_last(0, pair)
        for q in range(2):
            tend_x[2 * pair + q + 1] = values[q]
        return carry

    lax.fori_loop(0, 3, last_x, 0)
    x_halo = halo(tend_x, 1, 4, False)
    for copy in x_halo:
        copy.start()

    fwd_wait(spec_w, got_w, 3, 6, 6)

    def last_y(pair, carry):
        values = z_last(1, pair)
        for q in range(2):
            cross[2 * pair + q] = turned(values[q]) * own_ky
        return carry

    lax.fori_loop(0, 3, last_y, 0)

    def last_z(pair, carry):
        fwd_wait(spec_w, got_w, 4 + pair, 12 + 2 * pair, 2)
        values = z_last(2, pair)
        for q in range(2):
            j = 2 * pair + q
            cross[j] = cross[j] + turned(values[q]) * wavez[...]
        return carry

    lax.fori_loop(0, 3, last_z, 0)

    def sweep_own(j):
        diverge[j + 1] = 0.5 * (tend_x[j + 2] - tend_x[j]) + cross[j]
        first[j + 1] = (guess[j + 3] + guess[j + 1] - diverge[j + 1]) * recip[...]

    for j in (1, 4):
        sweep_own(j)
    late[0] = 0.5 * tend_x[2] + cross[0]
    late[1] = first[2]
    late[2] = 0.5 * tend_x[5] - cross[5]
    late[3] = first[5]
    late_halo = (
        x_copy(late.at[pl.ds(0, 2)], late.at[pl.ds(6, 2)], 6, left),
        x_copy(late.at[pl.ds(2, 2)], late.at[pl.ds(4, 2)], 7, right),
    )
    for copy in late_halo:
        copy.start()
    for copy in x_halo:
        copy.wait_recv()
    rotate_ends(((tend_x, 0),), ((tend_x, planes + 1),))
    for j in (0, 2, 3, 5):
        sweep_own(j)

    def sweep_again(j):
        press[j + 1] = (first[j + 2] + first[j] - diverge[j + 1]) * recip[...]

    for j in (1, 2, 3, 4):
        sweep_again(j)
    loads[10].wait()

    def inv_copy(pair, c, dest):
        at = pair * 6 + c * 2
        return pltpu.make_async_remote_copy(
            src_ref=spatial.at[pl.ds(at, 2), own_rows(dest), :],
            dst_ref=got_s.at[pl.ds(at, 2), :, own_cols(me)],
            send_sem=inv_send.at[pair * 3 + c, dest],
            recv_sem=inv_recv.at[pair * 3 + c, me],
            device_id={"gx": gx, "yz": dest},
            device_id_type=MESH,
        )

    def inv_own(pair, c):
        at = pair * 6 + c * 2
        return pltpu.make_async_copy(
            spatial.at[pl.ds(at, 2), own_rows(me), :],
            got_s.at[pl.ds(at, 2), :, own_cols(me)],
            inv_recv.at[pair * 3 + c, me],
        )

    def finish(pair):
        for q in range(2):
            p = 2 * pair + q
            here = press[p + 1]
            side = turned(here)
            slopes = (0.5 * (press[p + 2] - press[p]), side * own_ky, side * wavez[...])
            for c in range(3):
                qold[c, p] = keep_weight * qold[c, p] + time_step * (
                    tend[c * planes + p] - slopes[c]
                )

        def back(c, carry):
            at = pair * 6 + c * 2
            values = z_join([z_pair(qold.at[c], 2 * pair, 3)])
            spatial[at] = values[0]
            spatial[at + 1] = values[1]

            def send(d, inner):
                inv_copy(pair, c, peer(d)).start()
                return inner

            lax.fori_loop(1, GROUPS, send, 0)
            inv_own(pair, c).start()
            return carry

        lax.fori_loop(0, 3, back, 0)

    finish(1)
    for copy in late_halo:
        copy.wait_recv()
    rotate_ends(((late, 4), (late, 5)), ((late, 6), (late, 7)))
    low = 0.5 * tend_x[1] - late[4]
    first[0] = (guess[2] + guess[0] - low) * recip[...]
    press[0] = (first[1] + late[5] - low) * recip[...]
    high = late[6] - 0.5 * tend_x[6]
    first[7] = (guess[9] + guess[7] - high) * recip[...]
    press[7] = (late[7] + first[6] - high) * recip[...]
    for j in (0, 5):
        sweep_again(j)

    def finish_ends(i, carry):
        finish(i * 2)
        return carry

    lax.fori_loop(0, 2, finish_ends, 0)

    def result(c, pair, slot):
        return pltpu.make_async_copy(
            spec_u.at[pl.ds(pair * 6 + 2 * c, 2)], vnext_hbm.at[c, pl.ds(2 * pair, 2)], out_sem.at[slot]
        )

    results = [
        pltpu.make_async_copy(press.at[pl.ds(1, planes)], pout_hbm, out_sem.at[0]),
        pltpu.make_async_copy(qold, qnext_hbm, out_sem.at[1]),
    ]
    for copy in results:
        copy.start()
    results += [result(c, pair, 2 + pair * 3 + c) for pair in range(3) for c in range(3)]

    def sent_u(d, carry):
        fwd_copy(spec_u, got_u, 0, peer(d), 0, 18).wait_send()
        return carry

    lax.fori_loop(1, GROUPS, sent_u, 0)

    rows_c = planes * rows

    def arrive(i, carry):
        pair = jnp.where(i == 0, 1, jnp.where(i == 1, 0, 2))
        for c in range(3):
            inv_own(pair, c).wait()

            def step(d, inner, c=c):
                src = peer(d)
                where = got_s.at[pl.ds(pair * 6 + c * 2, 2), :, own_cols(src)]
                pltpu.make_async_remote_copy(
                    src_ref=where, dst_ref=where, send_sem=inv_send.at[pair * 3 + c, src],
                    recv_sem=inv_recv.at[pair * 3 + c, src], device_id={"gx": gx, "yz": src},
                    device_id_type=MESH,
                ).wait_recv()
                return inner

            lax.fori_loop(1, GROUPS, step, 0)
        high, low = split(got_s[pl.ds(pair * 6, 6)].reshape(rows_c, width))
        left_side[0:rows_c, :] = high
        left_side[rows_c : 2 * rows_c, :] = low

        def cells(k, inner):
            cols = pl.ds(pl.multiple_of(k * 256, 256), 256)
            both = mm(left_side[0 : 2 * rows_c, :], f_hi[:, cols])
            out = both[:rows_c] + both[rows_c:] + mm(left_side[0:rows_c, :], f_lo[:, cols])
            for c in range(3):
                for q in range(2):
                    at = (c * 2 + q) * rows
                    p = 2 * pair + q
                    spec_u[pair * 6 + 2 * c + q, :, cols] = (
                        ghost[c, p + 3, :, cols] + out[at : at + rows]
                    )
            return inner

        lax.fori_loop(0, 4, cells, 0)
        for c in range(3):
            result(c, pair, 2 + pair * 3 + c).start()
        return carry

    lax.fori_loop(0, 3, arrive, 0)

    def drain(d, carry):
        dest = peer(d)
        fwd_copy(spec_c, got_c, 1, dest, 0, 18).wait_send()
        for kind, at, count in w_parts:
            fwd_copy(spec_w, got_w, kind, dest, at, count).wait_send()
        for pair in range(3):
            for c in range(3):
                inv_copy(pair, c, dest).wait_send()
        return carry

    lax.fori_loop(1, GROUPS, drain, 0)
    if relayed:
        for i, ends, helps in ((0, ends_left, helps_left), (1, ends_right, helps_right)):

            @pl.when(ends)
            def _():
                to_relay[i].wait_send()
                near_halo[i].wait_send()

            @pl.when(jnp.logical_not(ends))
            def _():
                vel_halo[i].wait_send()

            @pl.when(helps)
            def _():
                from_relay[i].wait_send()

    else:
        for copy in vel_halo:
            copy.wait_send()
    for copy in guess_halo + x_halo + late_halo:
        copy.wait_send()
    for copy in results:
        copy.wait()


def move(*refs):
    v_in, q_in, p_in, v_out, q_out, p_out, v, q, p, sem_in, sem_out = refs
    legs = []
    for c in range(3):
        legs.append((v_in.at[c], v.at[c], v_out.at[c]))
        legs.append((q_in.at[c], q.at[c], q_out.at[c]))
    legs.append((p_in, p, p_out))
    into = [pltpu.make_async_copy(a, b, sem_in.at[i]) for i, (a, b, _) in enumerate(legs)]
    out = [pltpu.make_async_copy(b, c, sem_out.at[i]) for i, (_, b, c) in enumerate(legs)]
    for copy in into:
        copy.start()
    for first, second in zip(into, out):
        first.wait()
        second.start()
    for copy in out:
        copy.wait()


def local(slabs, vel, q_old, pressure_guess, shear_shift):
    width = vel.shape[3]
    depth = q_old.shape[2]
    half = width // (2 * GROUPS)
    planes, rows = vel.shape[1], vel.shape[2]
    consts = tables(width, depth)
    modes = lax.axis_index("yz") * half + jnp.arange(2 * half, dtype=jnp.int32) % half
    angle = (2.0 * math.pi / width) * (
        (modes * shear_shift[0] % width).astype(F32) + fraction * modes.astype(F32)
    )
    edge = jnp.stack([jnp.cos(angle), jnp.sin(angle)])
    any_spec = pl.BlockSpec(memory_space=pl.ANY)
    vmem = lambda *shape: pltpu.VMEM(shape, F32)
    wide = lambda n: pltpu.VMEM((n, depth, 2 * half), F32)
    flat = 3 * planes * rows
    scratch = [
        vmem(3, planes + 6, rows, width),
        vmem(3, 3, rows, width - 384),
        vmem(*consts[0].shape),
        vmem(2, *consts[1].shape),
        vmem(*consts[2].shape),
        vmem(*consts[3].shape),
        vmem(*consts[4].shape),
        vmem(*consts[5].shape),
        pltpu.VMEM(consts[6].shape, BF16),
        vmem(2, 2 * half),
        vmem(3, planes, depth, 2 * half),
        pltpu.VMEM((width, width), BF16),
        pltpu.VMEM((width, width), BF16),
        pltpu.VMEM((4 * flat, width), BF16),
        vmem(3 * planes, rows, width),
        vmem(3 * planes, rows, width),
        vmem(3 * planes, rows, width),
        wide(3 * planes),
        wide(3 * planes),
        wide(3 * planes),
        wide(3 * planes),
        wide(planes + 2),
        wide(planes),
        wide(planes + 4),
        wide(8),
        vmem(depth, 2 * half),
        wide(planes + 2),
        wide(planes + 2),
        wide(planes + 2),
        wide(3 * planes),
        vmem(3 * planes, rows, width),
        pltpu.SemaphoreType.DMA((11,)),
        pltpu.SemaphoreType.DMA((10,)),
        pltpu.SemaphoreType.DMA((10,)),
        pltpu.SemaphoreType.DMA((7, GROUPS)),
        pltpu.SemaphoreType.DMA((7, GROUPS)),
        pltpu.SemaphoreType.DMA((9, GROUPS)),
        pltpu.SemaphoreType.DMA((9, GROUPS)),
        pltpu.SemaphoreType.DMA((11,)),
    ]
    call = pl.pallas_call(
        functools.partial(body, slabs),
        out_shape=(
            jax.ShapeDtypeStruct(vel.shape, F32),
            jax.ShapeDtypeStruct(q_old.shape, F32),
            jax.ShapeDtypeStruct(pressure_guess.shape, F32),
        ),
        in_specs=[pl.BlockSpec(memory_space=pltpu.SMEM)] + [any_spec] * 11,
        out_specs=(any_spec, any_spec, any_spec),
        scratch_shapes=scratch,
        compiler_params=pltpu.CompilerParams(
            collective_id=0, has_side_effects=True, vmem_limit_bytes=63 * 2**20
        ),
        name="section",
    )
    out = call(shear_shift, vel, q_old, pressure_guess, edge, *consts)
    return pl.pallas_call(
        move,
        out_shape=tuple(jax.ShapeDtypeStruct(v.shape, F32) for v in out),
        in_specs=[any_spec] * 3,
        out_specs=(any_spec, any_spec, any_spec),
        scratch_shapes=[pltpu.VMEM(v.shape, F32) for v in out]
        + [pltpu.SemaphoreType.DMA((7,)), pltpu.SemaphoreType.DMA((7,))],
        compiler_params=pltpu.CompilerParams(vmem_limit_bytes=63 * 2**20),
        name="move",
    )(*out)


def solution(mesh):
    in_specs = (P(None, "gx", "yz", None), P(None, "gx", None, "yz"), P("gx", None, "yz"), P())
    out_specs = (P(None, "gx", "yz", None), P(None, "gx", None, "yz"), P("gx", None, "yz"))
    return jax.shard_map(
        functools.partial(local, mesh.shape["gx"]),
        mesh=mesh, in_specs=in_specs, out_specs=out_specs, check_vma=False,
    )
```

```python
import functools
import math

import jax
import jax.numpy as jnp
import numpy as np
from jax import lax
from jax.experimental import pallas as pl
from jax.experimental.pallas import tpu as pltpu
from jax.sharding import PartitionSpec as P

viscosity = 0.05
time_step = 0.2
keep_weight = -5.0 / 9.0
section_weight = 15.0 / 16.0
shear_param = 1.5
fraction = 0.375
GROUPS = 8
MESH = pl.DeviceIdType.MESH
F32 = jnp.float32
BF16 = jnp.bfloat16


def tables(width_y, depth_z):
    half = width_y // (2 * GROUPS)
    lanes = np.arange(width_y)
    mode = lanes // (2 * half) * half + lanes % half
    is_im = (lanes // half) % 2 == 1
    coarse = np.arange(width_y // half)
    fine = np.arange(half)

    def angle(n, k):
        return 2.0 * np.pi / width_y * ((n[:, None] * k[None, :]) % width_y)

    scale = 1.0 / math.sqrt(width_y)
    alpha = angle(coarse * half, mode)
    beta = angle(fine, mode)
    fwd_coarse = np.concatenate([np.cos(alpha), np.sin(alpha)])
    fwd_fine = scale * np.where(is_im[None], -np.sin(beta), np.cos(beta))
    cells = np.arange(width_y)
    alpha = angle(np.arange(GROUPS) * half, cells)
    beta = angle(fine, cells)
    inv_coarse = np.concatenate([np.cos(alpha), np.sin(alpha)])
    inv_fine = (2.0 * section_weight * scale) * np.stack([np.cos(beta), -np.sin(beta)])
    wave_y = 2.0 * np.pi / width_y * mode[None, :]
    m = np.arange(depth_z)
    signed = np.where(m < depth_z // 2, m, m - depth_z)
    wave_z = (2.0 * np.pi / depth_z * signed)[:, None]
    angle_z = 2.0 * np.pi / depth_z * ((m[:, None] * m[None, :]) % depth_z)
    forward = np.exp(-1j * angle_z) / math.sqrt(depth_z)
    mats = [
        forward,
        1j * wave_z * forward,
        -viscosity * wave_z * wave_z * forward,
        np.exp(1j * angle_z) / math.sqrt(depth_z),
    ]
    stacked = []
    for mat in mats:
        both = np.concatenate([mat.real, mat.imag]).astype(np.float32)
        high = both.astype(BF16)
        low = (both - high.astype(np.float32)).astype(BF16)
        stacked.append(np.concatenate([high, low]))
    as32 = lambda v: jnp.asarray(np.asarray(v, np.float32))
    return (
        as32(fwd_coarse),
        as32(fwd_fine),
        as32(inv_coarse),
        as32(inv_fine),
        as32(wave_y),
        as32(np.broadcast_to(wave_z, (depth_z, 2 * half))),
        jnp.asarray(np.stack(stacked)),
    )


def split(value):
    high = value.astype(BF16)
    low = (value - high.astype(F32)).astype(BF16)
    return high, low


def mm(a, b):
    return jnp.dot(a, b, preferred_element_type=F32)


def body(
    slabs,
    shift_ref,
    vel_hbm,
    qold_hbm,
    guess_hbm,
    cos_hbm,
    sin_hbm,
    fcoarse_hbm,
    ffine_hbm,
    icoarse_hbm,
    ifine_hbm,
    wavey_hbm,
    wavez_hbm,
    zmat_hbm,
    vnext_hbm,
    qnext_hbm,
    pout_hbm,
    ghost,
    relay,
    fcoarse,
    ffine,
    icoarse,
    ifine,
    wavey,
    wavez,
    zmat,
    edge,
    qold,
    f_hi,
    f_lo,
    left_side,
    spec_u,
    spec_c,
    spec_w,
    got_u,
    got_c,
    got_w,
    tend,
    tend_x,
    cross,
    guess,
    late,
    recip,
    diverge,
    first,
    press,
    spatial,
    got_s,
    load_sem,
    halo_send,
    halo_recv,
    fwd_send,
    fwd_recv,
    inv_send,
    inv_recv,
    out_sem,
):
    gx = lax.axis_index("gx")
    me = lax.axis_index("yz")
    my_z = me // 2
    right = lax.rem(gx + 1, slabs)
    left = lax.rem(gx + slabs - 1, slabs)
    relayed = slabs == 16
    near = 384
    planes = 6
    rows = 24
    width = 1024
    depth = 192
    lanes = 128
    half = 64
    flat = planes * rows * 3

    def peer(d):
        return lax.rem(me + d, GROUPS)

    def own_cols(ref_index):
        return pl.ds(pl.multiple_of(ref_index * lanes, lanes), lanes)

    def own_rows(ref_index):
        return pl.ds(pl.multiple_of(ref_index * rows, 8), rows)

    loads = [
        (vel_hbm, ghost.at[:, pl.ds(3, planes)]),
        (fcoarse_hbm, fcoarse),
        (ffine_hbm, ffine.at[0]),
        (guess_hbm, guess.at[pl.ds(1, planes)]),
        (wavey_hbm, wavey),
        (cos_hbm, edge.at[0]),
        (sin_hbm, edge.at[1]),
        (zmat_hbm, zmat),
        (wavez_hbm, wavez),
        (icoarse_hbm, icoarse),
        (ifine_hbm, ifine),
        (qold_hbm, qold),
    ]
    loads = [pltpu.make_async_copy(s, d, load_sem.at[i]) for i, (s, d) in enumerate(loads)]
    for i in (1, 2, 0, 3, 4, 5, 6, 7, 8, 9, 10, 11):
        loads[i].start()

    barrier = pltpu.get_barrier_semaphore()
    for d in range(1, GROUPS):
        pl.semaphore_signal(
            barrier, inc=1, device_id={"gx": gx, "yz": peer(d)}, device_id_type=MESH
        )
    for side in (left, right):
        pl.semaphore_signal(barrier, inc=1, device_id={"gx": side, "yz": me}, device_id_type=MESH)
    place = lax.rem(gx, 8)
    ends_right = place == 7
    ends_left = place == 0
    helps_left = place == 3
    helps_right = place == 4
    helper = ends_right | ends_left | helps_left | helps_right
    far_side = lax.rem(gx + jnp.where(ends_right | helps_left, 5, slabs - 5), slabs)
    near_side = lax.rem(gx + jnp.where(ends_right | helps_right, slabs - 4, 4), slabs)
    if relayed:

        @pl.when(helper)
        def _():
            for side in (far_side, near_side):
                pl.semaphore_signal(
                    barrier, inc=1, device_id={"gx": side, "yz": me}, device_id_type=MESH
                )

    def x_copy(src, dst, slot, target):
        return pltpu.make_async_remote_copy(
            src_ref=src, dst_ref=dst, send_sem=halo_send.at[slot], recv_sem=halo_recv.at[slot],
            device_id={"gx": target, "yz": me}, device_id_type=MESH,
        )

    def halo(ref, count, slot, lead):
        def at(start):
            return ref.at[:, pl.ds(start, count)] if lead else ref.at[pl.ds(start, count)]

        return (
            x_copy(at(count), at(count + planes), slot, left),
            x_copy(at(planes), at(0), slot + 1, right),
        )

    sign = jnp.where(lax.broadcasted_iota(jnp.int32, (1, lanes), 1) < half, -1.0, 1.0).astype(F32)

    def turned(value):
        return pltpu.roll(value, half, 1) * sign

    def store_split(at, value, gap=flat):
        high, low = split(value)
        left_side[pl.ds(pl.multiple_of(at, 48), 48), :] = high
        left_side[pl.ds(pl.multiple_of(at + gap, 48), 48), :] = low

    def build(col):
        cols = pl.ds(col, 256)
        for side in range(2):
            part = pl.ds(pl.multiple_of(col + side * lanes, lanes), lanes)
            ffine[1, :, part] = -turned(ffine[0, :, part])

        def step(a, carry):
            value = (
                fcoarse[pl.ds(a, 1), cols] * ffine[0, :, cols]
                + fcoarse[pl.ds(a + width // half, 1), cols] * ffine[1, :, cols]
            )
            high, low = split(value)
            where = pl.ds(pl.multiple_of(a * half, half), half)
            f_hi[where, cols] = high
            f_lo[where, cols] = low
            return carry

        lax.fori_loop(0, width // half, step, 0)

    def pairs_loop(write):
        def step(i, carry):
            write(i // 3, lax.rem(i, 3) * 2, i * 48)
            return carry

        lax.fori_loop(0, 9, step, 0)

    def to_modes(slot, col):
        cols = pl.ds(col, 256)
        both = mm(left_side[pl.ds(slot * 2 * flat, 2 * flat), :], f_hi[:, cols])
        low = mm(left_side[pl.ds(slot * 2 * flat, flat), :], f_lo[:, cols])
        return both[:flat] + both[flat:] + low

    def column(i):
        target = lax.rem(my_z + jnp.where(i == 0, 1, jnp.where(i == 1, 3, jnp.where(i == 2, 2, 0))), 4)
        return target, pl.multiple_of(target * 256, 256)

    def fwd_copy(spec, got, kind, dest, at, count):
        return pltpu.make_async_remote_copy(
            src_ref=spec.at[pl.ds(at, count), :, own_cols(dest)],
            dst_ref=got.at[pl.ds(at, count), own_rows(me), :],
            send_sem=fwd_send.at[kind, dest],
            recv_sem=fwd_recv.at[kind, me],
            device_id={"gx": gx, "yz": dest},
            device_id_type=MESH,
        )

    def fwd_own(spec, got, kind, at, count):
        return pltpu.make_async_copy(
            spec.at[pl.ds(at, count), :, own_cols(me)],
            got.at[pl.ds(at, count), own_rows(me), :],
            fwd_recv.at[kind, me],
        )

    def fwd_wait(spec, got, kind, at, count):
        fwd_own(spec, got, kind, at, count).wait()

        def step(d, carry):
            src = peer(d)
            where = got.at[pl.ds(at, count), own_rows(src), :]
            pltpu.make_async_remote_copy(
                src_ref=where, dst_ref=where, send_sem=fwd_send.at[kind, src],
                recv_sem=fwd_recv.at[kind, src], device_id={"gx": gx, "yz": src},
                device_id_type=MESH,
            ).wait_recv()
            return carry

        lax.fori_loop(1, GROUPS, step, 0)

    def send_column(spec, got, kind, i, at, count):
        target, _ = column(i)
        for side in range(2):
            dest = target * 2 + side

            @pl.when(dest != me)
            def _():
                fwd_copy(spec, got, kind, dest, at, count).start()

    def put_u(c, p, at):
        store_split(at, ghost[c, pl.ds(3 + p, 2)].reshape(48, width))

    def modes_of(spec, i, make):
        _, col = column(i)
        if make:
            build(col)
        spec[:, :, pl.ds(col, 256)] = to_modes(0, col).reshape(18, rows, 256)

    loads[1].wait()
    loads[2].wait()
    build(column(0)[1])
    loads[0].wait()
    pairs_loop(put_u)
    modes_of(spec_u, 0, False)
    loads[3].wait()
    vel_halo = halo(ghost, 3, 0, True)
    guess_halo = halo(guess, 1, 2, False)

    def part(ref, start, side):
        cols = pl.ds(0, near) if side == 0 else pl.ds(near, width - near)
        return ref.at[:, pl.ds(start, 3), :, cols]

    near_halo = (
        x_copy(part(ghost, 3, 0), part(ghost, planes + 3, 0), 0, left),
        x_copy(part(ghost, planes, 0), part(ghost, 0, 0), 1, right),
    )
    to_relay = (
        x_copy(part(ghost, 3, 1), relay, 8, far_side),
        x_copy(part(ghost, planes, 1), relay, 8, far_side),
    )
    from_relay = (
        x_copy(relay, part(ghost, planes + 3, 1), 9, near_side),
        x_copy(relay, part(ghost, 0, 1), 9, near_side),
    )

    if relayed:
        pl.semaphore_wait(barrier, jnp.where(helper, GROUPS + 3, GROUPS + 1))
        for i, ends in ((0, ends_left), (1, ends_right)):

            @pl.when(ends)
            def _():
                to_relay[i].start()
                near_halo[i].start()

            @pl.when(jnp.logical_not(ends))
            def _():
                vel_halo[i].start()

    else:
        pl.semaphore_wait(barrier, GROUPS + 1)
        for copy in vel_halo:
            copy.start()
    for copy in guess_halo:
        copy.start()
    send_column(spec_u, got_u, 0, 0, 0, 18)

    def rest_u(i, carry):
        modes_of(spec_u, i, True)
        send_column(spec_u, got_u, 0, i, 0, 18)
        return carry

    lax.fori_loop(1, 4, rest_u, 0)
    fwd_own(spec_u, got_u, 0, 0, 18).start()

    def put_c(c, p, at):
        u_z = ghost[2, pl.ds(3 + p, 2)]
        store_split(at, (-u_z * ghost[c, pl.ds(3 + p, 2)]).reshape(48, width))

    pairs_loop(put_c)

    def all_c(i, carry):
        modes_of(spec_c, i, False)
        send_column(spec_c, got_c, 1, i, 0, 18)
        return carry

    lax.fori_loop(0, 4, all_c, 0)
    fwd_own(spec_c, got_c, 1, 0, 18).start()

    if relayed:
        for i, helps in ((0, helps_left), (1, helps_right)):

            @pl.when(helps)
            def _():
                to_relay[i].wait_recv()
                from_relay[i].start()

        for i, ends in ((0, ends_right), (1, ends_left)):

            @pl.when(ends)
            def _():
                near_halo[i].wait_recv()
                from_relay[i].wait_recv()

            @pl.when(jnp.logical_not(ends))
            def _():
                vel_halo[i].wait_recv()

    else:
        for copy in vel_halo:
            copy.wait_recv()
    shift = shift_ref[0]

    def fix(start, amount, extra):
        def step(i, carry):
            c, p = i // 3, lax.rem(i, 3) + start
            once = pltpu.roll(ghost[c, p], amount, 1)
            ghost[c, p] = (1.0 - fraction) * once + fraction * pltpu.roll(once, extra, 1)
            return carry

        lax.fori_loop(0, 9, step, 0)

    @pl.when(gx == 0)
    def _():
        fix(0, lax.rem(width - shift, width), width - 1)

    @pl.when(gx == slabs - 1)
    def _():
        fix(planes + 3, shift, 1)

    total_x = planes * slabs
    omega = 2.0 / total_x

    def put_ab(i, carry):
        c, p = i // 3, lax.rem(i, 3) * 2
        terms_a = []
        terms_b = []
        for q in range(2):
            at = p + q + 3
            u_x = [ghost[0, at + o] for o in range(-3, 4)]
            u_i = [ghost[c, at + o] for o in range(-3, 4)]
            prod = [x * y for x, y in zip(u_x, u_i)]
            slope = (
                (45.0 / 60.0) * (prod[4] - prod[2])
                - (9.0 / 60.0) * (prod[5] - prod[1])
                + (1.0 / 60.0) * (prod[6] - prod[0])
            )
            bend = (
                (2.0 / 180.0) * (u_i[6] + u_i[0])
                - (27.0 / 180.0) * (u_i[5] + u_i[1])
                + (270.0 / 180.0) * (u_i[4] + u_i[2])
                - (490.0 / 180.0) * u_i[3]
            )
            u_y = ghost[1, at]
            weight_y = jnp.where(c == 0, 2.0 * omega, 0.0).astype(F32)
            weight_x = jnp.where(c == 1, -(2.0 - shear_param) * omega, 0.0).astype(F32)
            terms_a.append(viscosity * bend - slope + (weight_y * u_y + weight_x * u_x[3]))
            place = (gx * planes + p + q).astype(F32) + 0.5 - total_x / 2.0
            background = -shear_param * omega * place
            terms_b.append(-(u_y + background) * u_i[3])
        store_split(i * 48, jnp.concatenate(terms_a, axis=0))
        store_split(2 * flat + i * 48, jnp.concatenate(terms_b, axis=0))
        return carry

    lax.fori_loop(0, 9, put_ab, 0)
    loads[4].wait()

    def combine(i, carry):
        _, col = column(i)
        ya = to_modes(0, col)
        yb = to_modes(1, col)
        for side in range(2):
            wide = pl.ds(pl.multiple_of(col + side * lanes, lanes), lanes)
            cut = slice(side * lanes, (side + 1) * lanes)
            ky = wavey[0:1, wide]
            yu = spec_u[:, :, wide].reshape(flat, lanes)
            out = ya[:, cut] + turned(yb[:, cut]) * ky - (viscosity * ky * ky) * yu
            spec_w[:, :, wide] = out.reshape(18, rows, lanes)
        return carry

    lax.fori_loop(0, 4, combine, 0)
    w_parts = ((2, 0, 6), (3, 6, 6), (4, 12, 2), (5, 14, 2), (6, 16, 2))
    for kind, at, count in w_parts:
        def send_w(i, carry, kind=kind, at=at, count=count):
            send_column(spec_w, got_w, kind, i, at, count)
            return carry

        lax.fori_loop(0, 4, send_w, 0)
        fwd_own(spec_w, got_w, kind, at, count).start()

    for i in (5, 6, 7, 8, 9, 10):
        loads[i].wait()
    own_ky = wavey[0:1, own_cols(me)]
    recip[...] = 1.0 / (2.0 + own_ky * own_ky + wavez[...] * wavez[...])

    def build_back(g, carry):
        cosine = icoarse[pl.ds(g, 1), :]
        sine = icoarse[pl.ds(g + GROUPS, 1), :]
        for part in range(2):
            if part == 0:
                value = cosine * ifine[0] + sine * ifine[1]
            else:
                value = cosine * ifine[1] - sine * ifine[0]
            high, low = split(value)
            where = pl.ds(pl.multiple_of(g * lanes + part * half, half), half)
            f_hi[where, :] = high
            f_lo[where, :] = low
        return carry

    lax.fori_loop(0, GROUPS, build_back, 0)
    top = lax.broadcasted_iota(jnp.int32, (16, width), 0) == 0
    for table in (f_hi, f_lo):
        lines = table[0:16, :].astype(F32)
        table[0:16, :] = jnp.where(top, lines * 0.5, lines).astype(BF16)

    cosine = edge[0]
    sine = edge[1]

    def rotate_ends(lower, upper):
        @pl.when(gx == 0)
        def _():
            for ref, j in lower:
                value = ref[j]
                ref[j] = value * cosine + turned(value) * sine

        @pl.when(gx == slabs - 1)
        def _():
            for ref, j in upper:
                value = ref[j]
                ref[j] = value * cosine - turned(value) * sine

    for copy in guess_halo:
        copy.wait_recv()
    rotate_ends(((guess, 0),), ((guess, planes + 1),))

    def z_pair(ref, at, kind):
        value = jnp.concatenate([ref[at], ref[at + 1]], axis=1)
        high, low = split(value)
        return mm(zmat[kind], high), mm(zmat[kind, pl.ds(0, 2 * depth)], low)

    def z_join(parts):
        total = sum(wide[: 2 * depth] + wide[2 * depth :] + low for wide, low in parts)
        out = []
        for q in range(2):
            cut = slice(q * lanes, (q + 1) * lanes)
            out.append(total[:depth, cut] + turned(total[depth:, cut]))
        return out

    fwd_wait(spec_u, got_u, 0, 0, 18)
    fwd_wait(spec_c, got_c, 1, 0, 18)

    def z_first(i, carry):
        at = i * 2
        values = z_join([z_pair(got_c, at, 1), z_pair(got_u, at, 2)])
        tend[at] = values[0]
        tend[at + 1] = values[1]
        return carry

    lax.fori_loop(0, 9, z_first, 0)

    def z_last(c, pair):
        at = c * planes + pair * 2
        values = z_join([z_pair(got_w, at, 0)])
        for q in range(2):
            value = tend[at + q] + values[q]
            tend[at + q] = value
            values[q] = value
        return values

    fwd_wait(spec_w, got_w, 2, 0, 6)

    def last_x(pair, carry):
        values = z_last(0, pair)
        for q in range(2):
            tend_x[2 * pair + q + 1] = values[q]
        return carry

    lax.fori_loop(0, 3, last_x, 0)
    x_halo = halo(tend_x, 1, 4, False)
    for copy in x_halo:
        copy.start()

    fwd_wait(spec_w, got_w, 3, 6, 6)

    def last_y(pair, carry):
        values = z_last(1, pair)
        for q in range(2):
            cross[2 * pair + q] = turned(values[q]) * own_ky
        return carry

    lax.fori_loop(0, 3, last_y, 0)

    def last_z(pair, carry):
        fwd_wait(spec_w, got_w, 4 + pair, 12 + 2 * pair, 2)
        values = z_last(2, pair)
        for q in range(2):
            j = 2 * pair + q
            cross[j] = cross[j] + turned(values[q]) * wavez[...]
        return carry

    lax.fori_loop(0, 3, last_z, 0)

    def sweep_own(j):
        diverge[j + 1] = 0.5 * (tend_x[j + 2] - tend_x[j]) + cross[j]
        first[j + 1] = (guess[j + 2] + guess[j] - diverge[j + 1]) * recip[...]

    for j in (1, 4):
        sweep_own(j)
    low = 0.5 * tend_x[2] + cross[0]
    high = 0.5 * tend_x[5] - cross[5]
    late[0] = guess[2] - low
    late[1] = first[2] - low
    late[2] = guess[5] + high
    late[3] = first[5] + high
    late_halo = (
        x_copy(late.at[pl.ds(0, 2)], late.at[pl.ds(6, 2)], 6, left),
        x_copy(late.at[pl.ds(2, 2)], late.at[pl.ds(4, 2)], 7, right),
    )
    for copy in late_halo:
        copy.start()
    for copy in x_halo:
        copy.wait_recv()
    rotate_ends(((tend_x, 0),), ((tend_x, planes + 1),))
    for j in (0, 2, 3, 5):
        sweep_own(j)

    def sweep_again(j):
        press[j + 1] = (first[j + 2] + first[j] - diverge[j + 1]) * recip[...]

    for j in (1, 2, 3, 4):
        sweep_again(j)
    loads[11].wait()

    def inv_copy(pair, c, dest):
        at = pair * 6 + c * 2
        return pltpu.make_async_remote_copy(
            src_ref=spatial.at[pl.ds(at, 2), own_rows(dest), :],
            dst_ref=got_s.at[pl.ds(at, 2), :, own_cols(me)],
            send_sem=inv_send.at[pair * 3 + c, dest],
            recv_sem=inv_recv.at[pair * 3 + c, me],
            device_id={"gx": gx, "yz": dest},
            device_id_type=MESH,
        )

    def inv_own(pair, c):
        at = pair * 6 + c * 2
        return pltpu.make_async_copy(
            spatial.at[pl.ds(at, 2), own_rows(me), :],
            got_s.at[pl.ds(at, 2), :, own_cols(me)],
            inv_recv.at[pair * 3 + c, me],
        )

    def finish(pair):
        for q in range(2):
            p = 2 * pair + q
            here = press[p + 1]
            side = turned(here)
            slopes = (0.5 * (press[p + 2] - press[p]), side * own_ky, side * wavez[...])
            for c in range(3):
                qold[c, p] = keep_weight * qold[c, p] + time_step * (
                    tend[c * planes + p] - slopes[c]
                )

        def back(c, carry):
            at = pair * 6 + c * 2
            values = z_join([z_pair(qold.at[c], 2 * pair, 3)])
            spatial[at] = values[0]
            spatial[at + 1] = values[1]

            def send(d, inner):
                inv_copy(pair, c, peer(d)).start()
                return inner

            lax.fori_loop(1, GROUPS, send, 0)
            inv_own(pair, c).start()
            return carry

        lax.fori_loop(0, 3, back, 0)

    finish(1)
    for copy in late_halo:
        copy.wait_recv()
    rotate_ends(((late, 4), (late, 5)), ((late, 6), (late, 7)))
    low = 0.5 * tend_x[1]
    first[0] = (guess[1] + late[4] - low) * recip[...]
    press[0] = (first[1] + late[5] - low) * recip[...]
    high = 0.5 * tend_x[6]
    first[7] = (guess[6] + late[6] + high) * recip[...]
    press[7] = (first[6] + late[7] + high) * recip[...]
    for j in (0, 5):
        sweep_again(j)

    def finish_ends(i, carry):
        finish(i * 2)
        return carry

    lax.fori_loop(0, 2, finish_ends, 0)

    def result(c, pair, slot):
        return pltpu.make_async_copy(
            spec_u.at[pl.ds(pair * 6 + 2 * c, 2)], vnext_hbm.at[c, pl.ds(2 * pair, 2)], out_sem.at[slot]
        )

    results = [
        pltpu.make_async_copy(press.at[pl.ds(1, planes)], pout_hbm, out_sem.at[0]),
        pltpu.make_async_copy(qold, qnext_hbm, out_sem.at[1]),
    ]
    for copy in results:
        copy.start()
    results += [result(c, pair, 2 + pair * 3 + c) for pair in range(3) for c in range(3)]

    def sent_u(d, carry):
        fwd_copy(spec_u, got_u, 0, peer(d), 0, 18).wait_send()
        return carry

    lax.fori_loop(1, GROUPS, sent_u, 0)

    rows_c = 2 * rows

    def arrive(i, carry):
        c = lax.rem(i, 3)
        pair = jnp.where(i < 3, 1, jnp.where(i < 6, 0, 2))
        at = pair * 6 + c * 2
        inv_own(pair, c).wait()

        def step(d, inner):
            src = peer(d)
            where = got_s.at[pl.ds(at, 2), :, own_cols(src)]
            pltpu.make_async_remote_copy(
                src_ref=where, dst_ref=where, send_sem=inv_send.at[pair * 3 + c, src],
                recv_sem=inv_recv.at[pair * 3 + c, src], device_id={"gx": gx, "yz": src},
                device_id_type=MESH,
            ).wait_recv()
            return inner

        lax.fori_loop(1, GROUPS, step, 0)
        high, low = split(got_s[pl.ds(at, 2)].reshape(rows_c, width))
        left_side[0:rows_c, :] = high
        left_side[rows_c : 2 * rows_c, :] = low

        def cells(k, inner):
            cols = pl.ds(pl.multiple_of(k * 256, 256), 256)
            both = mm(left_side[0 : 2 * rows_c, :], f_hi[:, cols])
            out = both[:rows_c] + both[rows_c:] + mm(left_side[0:rows_c, :], f_lo[:, cols])
            spec_u[pl.ds(at, 2), :, cols] = (
                ghost[c, pl.ds(3 + 2 * pair, 2), :, cols] + out.reshape(2, rows, 256)
            )
            return inner

        lax.fori_loop(0, 4, cells, 0)
        result(c, pair, 2 + pair * 3 + c).start()
        return carry

    lax.fori_loop(0, 9, arrive, 0)

    def drain(d, carry):
        dest = peer(d)
        fwd_copy(spec_c, got_c, 1, dest, 0, 18).wait_send()
        for kind, at, count in w_parts:
            fwd_copy(spec_w, got_w, kind, dest, at, count).wait_send()
        for pair in range(3):
            for c in range(3):
                inv_copy(pair, c, dest).wait_send()
        return carry

    lax.fori_loop(1, GROUPS, drain, 0)
    if relayed:
        for i, ends, helps in ((0, ends_left, helps_left), (1, ends_right, helps_right)):

            @pl.when(ends)
            def _():
                to_relay[i].wait_send()
                near_halo[i].wait_send()

            @pl.when(jnp.logical_not(ends))
            def _():
                vel_halo[i].wait_send()

            @pl.when(helps)
            def _():
                from_relay[i].wait_send()

    else:
        for copy in vel_halo:
            copy.wait_send()
    for copy in guess_halo + x_halo + late_halo:
        copy.wait_send()
    for copy in results:
        copy.wait()


def move(*refs):
    v_in, q_in, p_in, v_out, q_out, p_out, v, q, p, sem_in, sem_out = refs
    legs = []
    for c in range(3):
        legs.append((v_in.at[c], v.at[c], v_out.at[c]))
        legs.append((q_in.at[c], q.at[c], q_out.at[c]))
    legs.append((p_in, p, p_out))
    into = [pltpu.make_async_copy(a, b, sem_in.at[i]) for i, (a, b, _) in enumerate(legs)]
    out = [pltpu.make_async_copy(b, c, sem_out.at[i]) for i, (_, b, c) in enumerate(legs)]
    for copy in into:
        copy.start()
    for first, second in zip(into, out):
        first.wait()
        second.start()
    for copy in out:
        copy.wait()


def local(slabs, vel, q_old, pressure_guess, shear_shift):
    width = vel.shape[3]
    depth = q_old.shape[2]
    half = width // (2 * GROUPS)
    planes, rows = vel.shape[1], vel.shape[2]
    consts = tables(width, depth)
    modes = lax.axis_index("yz") * half + jnp.arange(2 * half, dtype=jnp.int32) % half
    angle = (2.0 * math.pi / width) * (
        (modes * shear_shift[0] % width).astype(F32) + fraction * modes.astype(F32)
    )
    edge = (jnp.cos(angle)[None], jnp.sin(angle)[None])
    any_spec = pl.BlockSpec(memory_space=pl.ANY)
    vmem = lambda *shape: pltpu.VMEM(shape, F32)
    wide = lambda n: pltpu.VMEM((n, depth, 2 * half), F32)
    flat = 3 * planes * rows
    scratch = [
        vmem(3, planes + 6, rows, width),
        vmem(3, 3, rows, width - 384),
        vmem(*consts[0].shape),
        vmem(2, *consts[1].shape),
        vmem(*consts[2].shape),
        vmem(*consts[3].shape),
        vmem(*consts[4].shape),
        vmem(*consts[5].shape),
        pltpu.VMEM(consts[6].shape, BF16),
        vmem(2, 1, 2 * half),
        vmem(3, planes, depth, 2 * half),
        pltpu.VMEM((width, width), BF16),
        pltpu.VMEM((width, width), BF16),
        pltpu.VMEM((4 * flat, width), BF16),
        vmem(3 * planes, rows, width),
        vmem(3 * planes, rows, width),
        vmem(3 * planes, rows, width),
        wide(3 * planes),
        wide(3 * planes),
        wide(3 * planes),
        wide(3 * planes),
        wide(planes + 2),
        wide(planes),
        wide(planes + 2),
        wide(8),
        vmem(depth, 2 * half),
        wide(planes + 2),
        wide(planes + 2),
        wide(planes + 2),
        wide(3 * planes),
        vmem(3 * planes, rows, width),
        pltpu.SemaphoreType.DMA((12,)),
        pltpu.SemaphoreType.DMA((10,)),
        pltpu.SemaphoreType.DMA((10,)),
        pltpu.SemaphoreType.DMA((7, GROUPS)),
        pltpu.SemaphoreType.DMA((7, GROUPS)),
        pltpu.SemaphoreType.DMA((9, GROUPS)),
        pltpu.SemaphoreType.DMA((9, GROUPS)),
        pltpu.SemaphoreType.DMA((11,)),
    ]
    call = pl.pallas_call(
        functools.partial(body, slabs),
        out_shape=(
            jax.ShapeDtypeStruct(vel.shape, F32),
            jax.ShapeDtypeStruct(q_old.shape, F32),
            jax.ShapeDtypeStruct(pressure_guess.shape, F32),
        ),
        in_specs=[pl.BlockSpec(memory_space=pltpu.SMEM)] + [any_spec] * 12,
        out_specs=(any_spec, any_spec, any_spec),
        scratch_shapes=scratch,
        compiler_params=pltpu.CompilerParams(
            collective_id=0, has_side_effects=True, vmem_limit_bytes=63 * 2**20
        ),
        name="section",
    )
    out = call(shear_shift, vel, q_old, pressure_guess, *edge, *consts)
    return pl.pallas_call(
        move,
        out_shape=tuple(jax.ShapeDtypeStruct(v.shape, F32) for v in out),
        in_specs=[any_spec] * 3,
        out_specs=(any_spec, any_spec, any_spec),
        scratch_shapes=[pltpu.VMEM(v.shape, F32) for v in out]
        + [pltpu.SemaphoreType.DMA((7,)), pltpu.SemaphoreType.DMA((7,))],
        compiler_params=pltpu.CompilerParams(vmem_limit_bytes=63 * 2**20),
        name="move",
    )(*out)


def solution(mesh):
    in_specs = (P(None, "gx", "yz", None), P(None, "gx", None, "yz"), P("gx", None, "yz"), P())
    out_specs = (P(None, "gx", "yz", None), P(None, "gx", None, "yz"), P("gx", None, "yz"))
    return jax.shard_map(
        functools.partial(local, mesh.shape["gx"]),
        mesh=mesh, in_specs=in_specs, out_specs=out_specs, check_vma=False,
    )
```

```python
import functools
import math

import jax
import jax.numpy as jnp
import numpy as np
from jax import lax
from jax.experimental import pallas as pl
from jax.experimental.pallas import tpu as pltpu
from jax.sharding import PartitionSpec as P

viscosity = 0.05
time_step = 0.2
keep_weight = -5.0 / 9.0
section_weight = 15.0 / 16.0
shear_param = 1.5
fraction = 0.375
GROUPS = 8
MESH = pl.DeviceIdType.MESH
F32 = jnp.float32
BF16 = jnp.bfloat16


def tables(width_y, depth_z):
    half = width_y // (2 * GROUPS)
    lanes = np.arange(width_y)
    mode = lanes // (2 * half) * half + lanes % half
    is_im = (lanes // half) % 2 == 1
    coarse = np.arange(width_y // half)
    fine = np.arange(half)

    def angle(n, k):
        return 2.0 * np.pi / width_y * ((n[:, None] * k[None, :]) % width_y)

    scale = 1.0 / math.sqrt(width_y)
    alpha = angle(coarse * half, mode)
    beta = angle(fine, mode)
    fwd_coarse = np.concatenate([np.cos(alpha), np.sin(alpha)])
    fwd_fine = scale * np.where(is_im[None], -np.sin(beta), np.cos(beta))
    cells = np.arange(width_y)
    alpha = angle(np.arange(GROUPS) * half, cells)
    beta = angle(fine, cells)
    inv_coarse = np.concatenate([np.cos(alpha), np.sin(alpha)])
    inv_fine = (2.0 * section_weight * scale) * np.stack([np.cos(beta), -np.sin(beta)])
    wave_y = 2.0 * np.pi / width_y * mode[None, :]
    wave_y = np.concatenate([wave_y, np.cos(fraction * wave_y), np.sin(fraction * wave_y)])
    m = np.arange(depth_z)
    signed = np.where(m < depth_z // 2, m, m - depth_z)
    wave_z = (2.0 * np.pi / depth_z * signed)[:, None]
    angle_z = 2.0 * np.pi / depth_z * ((m[:, None] * m[None, :]) % depth_z)
    forward = np.exp(-1j * angle_z) / math.sqrt(depth_z)
    mats = [
        forward,
        1j * wave_z * forward,
        -viscosity * wave_z * wave_z * forward,
        np.exp(1j * angle_z) / math.sqrt(depth_z),
    ]
    stacked = []
    for mat in mats:
        both = np.concatenate([mat.real, mat.imag]).astype(np.float32)
        high = both.astype(BF16)
        low = (both - high.astype(np.float32)).astype(BF16)
        stacked.append(np.concatenate([high, low]))
    as32 = lambda v: jnp.asarray(np.asarray(v, np.float32))
    return (
        as32(fwd_coarse),
        as32(fwd_fine),
        as32(inv_coarse),
        as32(inv_fine),
        as32(wave_y),
        as32(np.broadcast_to(wave_z, (depth_z, 2 * half))),
        jnp.asarray(np.stack(stacked)),
    )


def split(value):
    high = value.astype(BF16)
    low = (value - high.astype(F32)).astype(BF16)
    return high, low


def mm(a, b):
    return jnp.dot(a, b, preferred_element_type=F32)


def body(
    slabs,
    shift_ref,
    vel_hbm,
    qold_hbm,
    guess_hbm,
    fcoarse_hbm,
    ffine_hbm,
    icoarse_hbm,
    ifine_hbm,
    wavey_hbm,
    wavez_hbm,
    zmat_hbm,
    vnext_hbm,
    qnext_hbm,
    pout_hbm,
    ghost,
    relay,
    fcoarse,
    ffine,
    icoarse,
    ifine,
    wavey,
    wavez,
    zmat,
    qold,
    f_hi,
    f_lo,
    left_side,
    spec_u,
    spec_c,
    spec_w,
    got_u,
    got_c,
    got_w,
    tend,
    tend_x,
    cross,
    guess,
    late,
    recip,
    diverge,
    first,
    press,
    spatial,
    got_s,
    load_sem,
    halo_send,
    halo_recv,
    fwd_send,
    fwd_recv,
    inv_send,
    inv_recv,
    out_sem,
):
    gx = lax.axis_index("gx")
    me = lax.axis_index("yz")
    my_z = me // 2
    right = lax.rem(gx + 1, slabs)
    left = lax.rem(gx + slabs - 1, slabs)
    relayed = slabs == 16
    near = 256
    planes = 6
    rows = 24
    width = 1024
    depth = 192
    lanes = 128
    half = 64
    flat = planes * rows * 3

    def peer(d):
        return lax.rem(me + d, GROUPS)

    def own_cols(ref_index):
        return pl.ds(pl.multiple_of(ref_index * lanes, lanes), lanes)

    def own_rows(ref_index):
        return pl.ds(pl.multiple_of(ref_index * rows, 8), rows)

    loads = [
        (vel_hbm, ghost.at[:, pl.ds(3, planes)]),
        (fcoarse_hbm, fcoarse),
        (ffine_hbm, ffine.at[0]),
        (guess_hbm, guess.at[pl.ds(1, planes)]),
        (wavey_hbm, wavey),
        (zmat_hbm, zmat),
        (wavez_hbm, wavez),
        (icoarse_hbm, icoarse),
        (ifine_hbm, ifine),
        (qold_hbm, qold),
    ]
    loads = [pltpu.make_async_copy(s, d, load_sem.at[i]) for i, (s, d) in enumerate(loads)]
    for i in (1, 2, 0, 3, 4, 5, 6, 7, 8, 9):
        loads[i].start()

    barrier = pltpu.get_barrier_semaphore()
    for d in range(1, GROUPS):
        pl.semaphore_signal(
            barrier, inc=1, device_id={"gx": gx, "yz": peer(d)}, device_id_type=MESH
        )
    for side in (left, right):
        pl.semaphore_signal(barrier, inc=1, device_id={"gx": side, "yz": me}, device_id_type=MESH)
    place = lax.rem(gx, 8)
    ends_right = place == 7
    ends_left = place == 0
    helps_left = place == 3
    helps_right = place == 4
    helper = ends_right | ends_left | helps_left | helps_right
    far_side = lax.rem(gx + jnp.where(ends_right | helps_left, 5, slabs - 5), slabs)
    near_side = lax.rem(gx + jnp.where(ends_right | helps_right, slabs - 4, 4), slabs)
    if relayed:

        @pl.when(helper)
        def _():
            for side in (far_side, near_side):
                pl.semaphore_signal(
                    barrier, inc=1, device_id={"gx": side, "yz": me}, device_id_type=MESH
                )

    def x_copy(src, dst, slot, target):
        return pltpu.make_async_remote_copy(
            src_ref=src, dst_ref=dst, send_sem=halo_send.at[slot], recv_sem=halo_recv.at[slot],
            device_id={"gx": target, "yz": me}, device_id_type=MESH,
        )

    def halo(ref, count, slot, lead):
        def at(start):
            return ref.at[:, pl.ds(start, count)] if lead else ref.at[pl.ds(start, count)]

        return (
            x_copy(at(count), at(count + planes), slot, left),
            x_copy(at(planes), at(0), slot + 1, right),
        )

    sign = jnp.where(lax.broadcasted_iota(jnp.int32, (1, lanes), 1) < half, -1.0, 1.0).astype(F32)

    def turned(value):
        return pltpu.roll(value, half, 1) * sign

    def store_split(at, value, gap=flat):
        high, low = split(value)
        left_side[pl.ds(pl.multiple_of(at, 48), 48), :] = high
        left_side[pl.ds(pl.multiple_of(at + gap, 48), 48), :] = low

    def build(col):
        cols = pl.ds(col, 256)
        for side in range(2):
            part = pl.ds(pl.multiple_of(col + side * lanes, lanes), lanes)
            ffine[1, :, part] = -turned(ffine[0, :, part])

        def step(a, carry):
            value = (
                fcoarse[pl.ds(a, 1), cols] * ffine[0, :, cols]
                + fcoarse[pl.ds(a + width // half, 1), cols] * ffine[1, :, cols]
            )
            high, low = split(value)
            where = pl.ds(pl.multiple_of(a * half, half), half)
            f_hi[where, cols] = high
            f_lo[where, cols] = low
            return carry

        lax.fori_loop(0, width // half, step, 0)

    def pairs_loop(write):
        def step(i, carry):
            write(i // 3, lax.rem(i, 3) * 2, i * 48)
            return carry

        lax.fori_loop(0, 9, step, 0)

    def to_modes(slot, col):
        cols = pl.ds(col, 256)
        both = mm(left_side[pl.ds(slot * 2 * flat, 2 * flat), :], f_hi[:, cols])
        low = mm(left_side[pl.ds(slot * 2 * flat, flat), :], f_lo[:, cols])
        return both[:flat] + both[flat:] + low

    def column(i):
        target = lax.rem(my_z + jnp.where(i == 0, 1, jnp.where(i == 1, 3, jnp.where(i == 2, 2, 0))), 4)
        return target, pl.multiple_of(target * 256, 256)

    def fwd_copy(spec, got, kind, dest, at, count):
        return pltpu.make_async_remote_copy(
            src_ref=spec.at[pl.ds(at, count), :, own_cols(dest)],
            dst_ref=got.at[pl.ds(at, count), own_rows(me), :],
            send_sem=fwd_send.at[kind, dest],
            recv_sem=fwd_recv.at[kind, me],
            device_id={"gx": gx, "yz": dest},
            device_id_type=MESH,
        )

    def fwd_own(spec, got, kind, at, count):
        return pltpu.make_async_copy(
            spec.at[pl.ds(at, count), :, own_cols(me)],
            got.at[pl.ds(at, count), own_rows(me), :],
            fwd_recv.at[kind, me],
        )

    def fwd_wait(spec, got, kind, at, count):
        fwd_own(spec, got, kind, at, count).wait()

        def step(d, carry):
            src = peer(d)
            where = got.at[pl.ds(at, count), own_rows(src), :]
            pltpu.make_async_remote_copy(
                src_ref=where, dst_ref=where, send_sem=fwd_send.at[kind, src],
                recv_sem=fwd_recv.at[kind, src], device_id={"gx": gx, "yz": src},
                device_id_type=MESH,
            ).wait_recv()
            return carry

        lax.fori_loop(1, GROUPS, step, 0)

    def send_column(spec, got, kind, i, at, count):
        target, _ = column(i)
        for side in range(2):
            dest = target * 2 + side

            @pl.when(dest != me)
            def _():
                fwd_copy(spec, got, kind, dest, at, count).start()

    def put_u(c, p, at):
        store_split(at, ghost[c, pl.ds(3 + p, 2)].reshape(48, width))

    def modes_of(spec, i, make):
        _, col = column(i)
        if make:
            build(col)
        spec[:, :, pl.ds(col, 256)] = to_modes(0, col).reshape(18, rows, 256)

    loads[1].wait()
    loads[2].wait()
    build(column(0)[1])
    loads[0].wait()
    pairs_loop(put_u)
    modes_of(spec_u, 0, False)
    loads[3].wait()
    vel_halo = halo(ghost, 3, 0, True)
    guess_halo = halo(guess, 1, 2, False)

    def part(ref, start, side):
        cols = pl.ds(0, near) if side == 0 else pl.ds(near, width - near)
        return ref.at[:, pl.ds(start, 3), :, cols]

    near_halo = (
        x_copy(part(ghost, 3, 0), part(ghost, planes + 3, 0), 0, left),
        x_copy(part(ghost, planes, 0), part(ghost, 0, 0), 1, right),
    )
    to_relay = (
        x_copy(part(ghost, 3, 1), relay, 8, far_side),
        x_copy(part(ghost, planes, 1), relay, 8, far_side),
    )
    from_relay = (
        x_copy(relay, part(ghost, planes + 3, 1), 9, near_side),
        x_copy(relay, part(ghost, 0, 1), 9, near_side),
    )

    if relayed:
        pl.semaphore_wait(barrier, jnp.where(helper, GROUPS + 3, GROUPS + 1))
        for i, ends in ((0, ends_left), (1, ends_right)):

            @pl.when(ends)
            def _():
                to_relay[i].start()
                near_halo[i].start()

            @pl.when(jnp.logical_not(ends))
            def _():
                vel_halo[i].start()

    else:
        pl.semaphore_wait(barrier, GROUPS + 1)
        for copy in vel_halo:
            copy.start()
    for copy in guess_halo:
        copy.start()
    send_column(spec_u, got_u, 0, 0, 0, 18)

    def rest_u(i, carry):
        modes_of(spec_u, i, True)
        send_column(spec_u, got_u, 0, i, 0, 18)
        return carry

    lax.fori_loop(1, 4, rest_u, 0)
    fwd_own(spec_u, got_u, 0, 0, 18).start()

    def put_c(c, p, at):
        u_z = ghost[2, pl.ds(3 + p, 2)]
        store_split(at, (-u_z * ghost[c, pl.ds(3 + p, 2)]).reshape(48, width))

    pairs_loop(put_c)

    def all_c(i, carry):
        modes_of(spec_c, i, False)
        send_column(spec_c, got_c, 1, i, 0, 18)
        return carry

    lax.fori_loop(0, 4, all_c, 0)
    fwd_own(spec_c, got_c, 1, 0, 18).start()

    if relayed:
        for i, helps in ((0, helps_left), (1, helps_right)):

            @pl.when(helps)
            def _():
                to_relay[i].wait_recv()
                from_relay[i].start()

        for i, ends in ((0, ends_right), (1, ends_left)):

            @pl.when(ends)
            def _():
                near_halo[i].wait_recv()
                from_relay[i].wait_recv()

            @pl.when(jnp.logical_not(ends))
            def _():
                vel_halo[i].wait_recv()

    else:
        for copy in vel_halo:
            copy.wait_recv()
    shift = shift_ref[0]

    def fix(start, amount, extra):
        def step(i, carry):
            c, p = i // 3, lax.rem(i, 3) + start
            once = pltpu.roll(ghost[c, p], amount, 1)
            ghost[c, p] = (1.0 - fraction) * once + fraction * pltpu.roll(once, extra, 1)
            return carry

        lax.fori_loop(0, 9, step, 0)

    @pl.when(gx == 0)
    def _():
        fix(0, lax.rem(width - shift, width), width - 1)

    @pl.when(gx == slabs - 1)
    def _():
        fix(planes + 3, shift, 1)

    total_x = planes * slabs
    omega = 2.0 / total_x

    def put_ab(i, carry):
        c, p = i // 3, lax.rem(i, 3) * 2
        terms_a = []
        terms_b = []
        for q in range(2):
            at = p + q + 3
            u_x = [ghost[0, at + o] for o in range(-3, 4)]
            u_i = [ghost[c, at + o] for o in range(-3, 4)]
            prod = [x * y for x, y in zip(u_x, u_i)]
            slope = (
                (45.0 / 60.0) * (prod[4] - prod[2])
                - (9.0 / 60.0) * (prod[5] - prod[1])
                + (1.0 / 60.0) * (prod[6] - prod[0])
            )
            bend = (
                (2.0 / 180.0) * (u_i[6] + u_i[0])
                - (27.0 / 180.0) * (u_i[5] + u_i[1])
                + (270.0 / 180.0) * (u_i[4] + u_i[2])
                - (490.0 / 180.0) * u_i[3]
            )
            u_y = ghost[1, at]
            weight_y = jnp.where(c == 0, 2.0 * omega, 0.0).astype(F32)
            weight_x = jnp.where(c == 1, -(2.0 - shear_param) * omega, 0.0).astype(F32)
            terms_a.append(viscosity * bend - slope + (weight_y * u_y + weight_x * u_x[3]))
            place = (gx * planes + p + q).astype(F32) + 0.5 - total_x / 2.0
            background = -shear_param * omega * place
            terms_b.append(-(u_y + background) * u_i[3])
        store_split(i * 48, jnp.concatenate(terms_a, axis=0))
        store_split(2 * flat + i * 48, jnp.concatenate(terms_b, axis=0))
        return carry

    lax.fori_loop(0, 9, put_ab, 0)
    loads[4].wait()

    def combine(i, carry):
        _, col = column(i)
        ya = to_modes(0, col)
        yb = to_modes(1, col)
        for side in range(2):
            wide = pl.ds(pl.multiple_of(col + side * lanes, lanes), lanes)
            cut = slice(side * lanes, (side + 1) * lanes)
            ky = wavey[0:1, wide]
            yu = spec_u[:, :, wide].reshape(flat, lanes)
            out = ya[:, cut] + turned(yb[:, cut]) * ky - (viscosity * ky * ky) * yu
            spec_w[:, :, wide] = out.reshape(18, rows, lanes)
        return carry

    lax.fori_loop(0, 4, combine, 0)
    w_parts = ((2, 0, 6), (3, 6, 6), (4, 12, 2), (5, 14, 2), (6, 16, 2))
    for kind, at, count in w_parts:
        def send_w(i, carry, kind=kind, at=at, count=count):
            send_column(spec_w, got_w, kind, i, at, count)
            return carry

        lax.fori_loop(0, 4, send_w, 0)
        fwd_own(spec_w, got_w, kind, at, count).start()

    for i in (5, 6, 7, 8):
        loads[i].wait()
    own_ky = wavey[0:1, own_cols(me)]
    recip[...] = 1.0 / (2.0 + own_ky * own_ky + wavez[...] * wavez[...])

    def build_back(g, carry):
        cosine = icoarse[pl.ds(g, 1), :]
        sine = icoarse[pl.ds(g + GROUPS, 1), :]
        for part in range(2):
            if part == 0:
                value = cosine * ifine[0] + sine * ifine[1]
            else:
                value = cosine * ifine[1] - sine * ifine[0]
            high, low = split(value)
            where = pl.ds(pl.multiple_of(g * lanes + part * half, half), half)
            f_hi[where, :] = high
            f_lo[where, :] = low
        return carry

    lax.fori_loop(0, GROUPS, build_back, 0)
    top = lax.broadcasted_iota(jnp.int32, (16, width), 0) == 0
    for table in (f_hi, f_lo):
        lines = table[0:16, :].astype(F32)
        table[0:16, :] = jnp.where(top, lines * 0.5, lines).astype(BF16)

    own = own_cols(me)
    coarse = shift // half
    fine = lax.rem(shift, half)
    real_lane = lax.broadcasted_iota(jnp.int32, (1, lanes), 1) < half

    def row_of(lines, row):
        there = lax.broadcasted_iota(jnp.int32, lines.shape, 0) == row
        return jnp.sum(jnp.where(there, lines, 0.0), axis=0, keepdims=True)

    first_row = row_of(ffine[0, :, own], fine)
    second_row = row_of(ffine[1, :, own], fine)
    unit = math.sqrt(width)
    cos_b = unit * jnp.where(real_lane, first_row, -second_row)
    sin_b = -unit * jnp.where(real_lane, second_row, first_row)
    cos_c, sin_c = wavey[1:2, own], wavey[2:3, own]
    cos_b, sin_b = cos_b * cos_c - sin_b * sin_c, sin_b * cos_c + cos_b * sin_c
    cos_c = row_of(fcoarse[0 : width // half, own], coarse)
    sin_c = row_of(fcoarse[width // half : 2 * width // half, own], coarse)
    cosine = cos_b * cos_c - sin_b * sin_c
    sine = sin_b * cos_c + cos_b * sin_c

    def rotate_ends(lower, upper):
        @pl.when(gx == 0)
        def _():
            for ref, j in lower:
                value = ref[j]
                ref[j] = value * cosine + turned(value) * sine

        @pl.when(gx == slabs - 1)
        def _():
            for ref, j in upper:
                value = ref[j]
                ref[j] = value * cosine - turned(value) * sine

    for copy in guess_halo:
        copy.wait_recv()
    rotate_ends(((guess, 0),), ((guess, planes + 1),))

    def z_pair(ref, at, kind):
        value = jnp.concatenate([ref[at], ref[at + 1]], axis=1)
        high, low = split(value)
        return mm(zmat[kind], high), mm(zmat[kind, pl.ds(0, 2 * depth)], low)

    def z_join(parts):
        total = sum(wide[: 2 * depth] + wide[2 * depth :] + low for wide, low in parts)
        out = []
        for q in range(2):
            cut = slice(q * lanes, (q + 1) * lanes)
            out.append(total[:depth, cut] + turned(total[depth:, cut]))
        return out

    fwd_wait(spec_u, got_u, 0, 0, 18)
    fwd_wait(spec_c, got_c, 1, 0, 18)

    def z_first(i, carry):
        at = i * 2
        values = z_join([z_pair(got_c, at, 1), z_pair(got_u, at, 2)])
        tend[at] = values[0]
        tend[at + 1] = values[1]
        return carry

    lax.fori_loop(0, 9, z_first, 0)

    def z_last(c, pair):
        at = c * planes + pair * 2
        values = z_join([z_pair(got_w, at, 0)])
        for q in range(2):
            value = tend[at + q] + values[q]
            tend[at + q] = value
            values[q] = value
        return values

    fwd_wait(spec_w, got_w, 2, 0, 6)

    def last_x(pair, carry):
        values = z_last(0, pair)
        for q in range(2):
            tend_x[2 * pair + q + 1] = values[q]
        return carry

    lax.fori_loop(0, 3, last_x, 0)
    x_halo = halo(tend_x, 1, 4, False)
    for copy in x_halo:
        copy.start()

    fwd_wait(spec_w, got_w, 3, 6, 6)

    def last_y(pair, carry):
        values = z_last(1, pair)
        for q in range(2):
            cross[2 * pair + q] = turned(values[q]) * own_ky
        return carry

    lax.fori_loop(0, 3, last_y, 0)

    def last_z(pair, carry):
        fwd_wait(spec_w, got_w, 4 + pair, 12 + 2 * pair, 2)
        values = z_last(2, pair)
        for q in range(2):
            j = 2 * pair + q
            cross[j] = cross[j] + turned(values[q]) * wavez[...]
        return carry

    lax.fori_loop(0, 3, last_z, 0)

    def sweep_own(j):
        diverge[j + 1] = 0.5 * (tend_x[j + 2] - tend_x[j]) + cross[j]
        first[j + 1] = (guess[j + 2] + guess[j] - diverge[j + 1]) * recip[...]

    for j in (1, 4):
        sweep_own(j)
    low = 0.5 * tend_x[2] + cross[0]
    high = 0.5 * tend_x[5] - cross[5]
    late[0] = guess[2] - low
    late[1] = first[2] - low
    late[2] = guess[5] + high
    late[3] = first[5] + high
    late_halo = (
        x_copy(late.at[pl.ds(0, 2)], late.at[pl.ds(6, 2)], 6, left),
        x_copy(late.at[pl.ds(2, 2)], late.at[pl.ds(4, 2)], 7, right),
    )
    for copy in late_halo:
        copy.start()
    for copy in x_halo:
        copy.wait_recv()
    rotate_ends(((tend_x, 0),), ((tend_x, planes + 1),))
    for j in (0, 2, 3, 5):
        sweep_own(j)

    def sweep_again(j):
        press[j + 1] = (first[j + 2] + first[j] - diverge[j + 1]) * recip[...]

    for j in (1, 2, 3, 4):
        sweep_again(j)
    loads[9].wait()

    def inv_copy(pair, c, dest):
        at = pair * 6 + c * 2
        return pltpu.make_async_remote_copy(
            src_ref=spatial.at[pl.ds(at, 2), own_rows(dest), :],
            dst_ref=got_s.at[pl.ds(at, 2), :, own_cols(me)],
            send_sem=inv_send.at[pair * 3 + c, dest],
            recv_sem=inv_recv.at[pair * 3 + c, me],
            device_id={"gx": gx, "yz": dest},
            device_id_type=MESH,
        )

    def inv_own(pair, c):
        at = pair * 6 + c * 2
        return pltpu.make_async_copy(
            spatial.at[pl.ds(at, 2), own_rows(me), :],
            got_s.at[pl.ds(at, 2), :, own_cols(me)],
            inv_recv.at[pair * 3 + c, me],
        )

    def finish(pair):
        for q in range(2):
            p = 2 * pair + q
            here = press[p + 1]
            side = turned(here)
            slopes = (0.5 * (press[p + 2] - press[p]), side * own_ky, side * wavez[...])
            for c in range(3):
                qold[c, p] = keep_weight * qold[c, p] + time_step * (
                    tend[c * planes + p] - slopes[c]
                )

        def back(c, carry):
            at = pair * 6 + c * 2
            values = z_join([z_pair(qold.at[c], 2 * pair, 3)])
            spatial[at] = values[0]
            spatial[at + 1] = values[1]

            def send(d, inner):
                inv_copy(pair, c, peer(d)).start()
                return inner

            lax.fori_loop(1, GROUPS, send, 0)
            inv_own(pair, c).start()
            return carry

        lax.fori_loop(0, 3, back, 0)

    finish(1)
    for copy in late_halo:
        copy.wait_recv()
    rotate_ends(((late, 4), (late, 5)), ((late, 6), (late, 7)))
    low = 0.5 * tend_x[1]
    first[0] = (guess[1] + late[4] - low) * recip[...]
    press[0] = (first[1] + late[5] - low) * recip[...]
    high = 0.5 * tend_x[6]
    first[7] = (guess[6] + late[6] + high) * recip[...]
    press[7] = (first[6] + late[7] + high) * recip[...]
    for j in (0, 5):
        sweep_again(j)

    def finish_ends(i, carry):
        finish(i * 2)
        return carry

    lax.fori_loop(0, 2, finish_ends, 0)

    def result(c, pair, slot):
        return pltpu.make_async_copy(
            spec_u.at[pl.ds(pair * 6 + 2 * c, 2)], vnext_hbm.at[c, pl.ds(2 * pair, 2)], out_sem.at[slot]
        )

    results = [
        pltpu.make_async_copy(press.at[pl.ds(1, planes)], pout_hbm, out_sem.at[0]),
        pltpu.make_async_copy(qold, qnext_hbm, out_sem.at[1]),
    ]
    for copy in results:
        copy.start()
    results += [result(c, pair, 2 + pair * 3 + c) for pair in range(3) for c in range(3)]

    def sent_u(d, carry):
        fwd_copy(spec_u, got_u, 0, peer(d), 0, 18).wait_send()
        return carry

    lax.fori_loop(1, GROUPS, sent_u, 0)

    rows_c = 2 * rows

    def arrive(i, carry):
        c = lax.rem(i, 3)
        pair = jnp.where(i < 3, 1, jnp.where(i < 6, 0, 2))
        at = pair * 6 + c * 2
        inv_own(pair, c).wait()

        def step(d, inner):
            src = peer(d)
            where = got_s.at[pl.ds(at, 2), :, own_cols(src)]
            pltpu.make_async_remote_copy(
                src_ref=where, dst_ref=where, send_sem=inv_send.at[pair * 3 + c, src],
                recv_sem=inv_recv.at[pair * 3 + c, src], device_id={"gx": gx, "yz": src},
                device_id_type=MESH,
            ).wait_recv()
            return inner

        lax.fori_loop(1, GROUPS, step, 0)
        high, low = split(got_s[pl.ds(at, 2)].reshape(rows_c, width))
        left_side[0:rows_c, :] = high
        left_side[rows_c : 2 * rows_c, :] = low

        def cells(k, inner):
            cols = pl.ds(pl.multiple_of(k * 512, 512), 512)
            both = mm(left_side[0 : 2 * rows_c, :], f_hi[:, cols])
            out = both[:rows_c] + both[rows_c:] + mm(left_side[0:rows_c, :], f_lo[:, cols])
            spec_u[pl.ds(at, 2), :, cols] = (
                ghost[c, pl.ds(3 + 2 * pair, 2), :, cols] + out.reshape(2, rows, 512)
            )
            return inner

        lax.fori_loop(0, 2, cells, 0)
        result(c, pair, 2 + pair * 3 + c).start()
        return carry

    lax.fori_loop(0, 9, arrive, 0)

    def drain(d, carry):
        dest = peer(d)
        fwd_copy(spec_c, got_c, 1, dest, 0, 18).wait_send()
        for kind, at, count in w_parts:
            fwd_copy(spec_w, got_w, kind, dest, at, count).wait_send()
        for pair in range(3):
            for c in range(3):
                inv_copy(pair, c, dest).wait_send()
        return carry

    lax.fori_loop(1, GROUPS, drain, 0)
    if relayed:
        for i, ends, helps in ((0, ends_left, helps_left), (1, ends_right, helps_right)):

            @pl.when(ends)
            def _():
                to_relay[i].wait_send()
                near_halo[i].wait_send()

            @pl.when(jnp.logical_not(ends))
            def _():
                vel_halo[i].wait_send()

            @pl.when(helps)
            def _():
                from_relay[i].wait_send()

    else:
        for copy in vel_halo:
            copy.wait_send()
    for copy in guess_halo + x_halo + late_halo:
        copy.wait_send()
    for copy in results:
        copy.wait()


def move(*refs):
    v_in, q_in, p_in, v_out, q_out, p_out, v, q, p, sem_in, sem_out = refs
    legs = []
    for c in range(3):
        legs.append((v_in.at[c], v.at[c], v_out.at[c]))
        legs.append((q_in.at[c], q.at[c], q_out.at[c]))
    legs.append((p_in, p, p_out))
    into = [pltpu.make_async_copy(a, b, sem_in.at[i]) for i, (a, b, _) in enumerate(legs)]
    out = [pltpu.make_async_copy(b, c, sem_out.at[i]) for i, (_, b, c) in enumerate(legs)]
    for copy in into:
        copy.start()
    for first, second in zip(into, out):
        first.wait()
        second.start()
    for copy in out:
        copy.wait()


def local(slabs, vel, q_old, pressure_guess, shear_shift):
    width = vel.shape[3]
    depth = q_old.shape[2]
    half = width // (2 * GROUPS)
    planes, rows = vel.shape[1], vel.shape[2]
    consts = tables(width, depth)
    any_spec = pl.BlockSpec(memory_space=pl.ANY)
    vmem = lambda *shape: pltpu.VMEM(shape, F32)
    wide = lambda n: pltpu.VMEM((n, depth, 2 * half), F32)
    flat = 3 * planes * rows
    scratch = [
        vmem(3, planes + 6, rows, width),
        vmem(3, 3, rows, width - 256),
        vmem(*consts[0].shape),
        vmem(2, *consts[1].shape),
        vmem(*consts[2].shape),
        vmem(*consts[3].shape),
        vmem(*consts[4].shape),
        vmem(*consts[5].shape),
        pltpu.VMEM(consts[6].shape, BF16),
        vmem(3, planes, depth, 2 * half),
        pltpu.VMEM((width, width), BF16),
        pltpu.VMEM((width, width), BF16),
        pltpu.VMEM((4 * flat, width), BF16),
        vmem(3 * planes, rows, width),
        vmem(3 * planes, rows, width),
        vmem(3 * planes, rows, width),
        wide(3 * planes),
        wide(3 * planes),
        wide(3 * planes),
        wide(3 * planes),
        wide(planes + 2),
        wide(planes),
        wide(planes + 2),
        wide(8),
        vmem(depth, 2 * half),
        wide(planes + 2),
        wide(planes + 2),
        wide(planes + 2),
        wide(3 * planes),
        vmem(3 * planes, rows, width),
        pltpu.SemaphoreType.DMA((10,)),
        pltpu.SemaphoreType.DMA((10,)),
        pltpu.SemaphoreType.DMA((10,)),
        pltpu.SemaphoreType.DMA((7, GROUPS)),
        pltpu.SemaphoreType.DMA((7, GROUPS)),
        pltpu.SemaphoreType.DMA((9, GROUPS)),
        pltpu.SemaphoreType.DMA((9, GROUPS)),
        pltpu.SemaphoreType.DMA((11,)),
    ]
    call = pl.pallas_call(
        functools.partial(body, slabs),
        out_shape=(
            jax.ShapeDtypeStruct(vel.shape, F32),
            jax.ShapeDtypeStruct(q_old.shape, F32),
            jax.ShapeDtypeStruct(pressure_guess.shape, F32),
        ),
        in_specs=[pl.BlockSpec(memory_space=pltpu.SMEM)] + [any_spec] * 10,
        out_specs=(any_spec, any_spec, any_spec),
        scratch_shapes=scratch,
        compiler_params=pltpu.CompilerParams(
            collective_id=0, has_side_effects=True, vmem_limit_bytes=63 * 2**20
        ),
        name="section",
    )
    out = call(shear_shift, vel, q_old, pressure_guess, *consts)
    return pl.pallas_call(
        move,
        out_shape=tuple(jax.ShapeDtypeStruct(v.shape, F32) for v in out),
        in_specs=[any_spec] * 3,
        out_specs=(any_spec, any_spec, any_spec),
        scratch_shapes=[pltpu.VMEM(v.shape, F32) for v in out]
        + [pltpu.SemaphoreType.DMA((7,)), pltpu.SemaphoreType.DMA((7,))],
        compiler_params=pltpu.CompilerParams(vmem_limit_bytes=63 * 2**20),
        name="move",
    )(*out)


def solution(mesh):
    in_specs = (P(None, "gx", "yz", None), P(None, "gx", None, "yz"), P("gx", None, "yz"), P())
    out_specs = (P(None, "gx", "yz", None), P(None, "gx", None, "yz"), P("gx", None, "yz"))
    return jax.shard_map(
        functools.partial(local, mesh.shape["gx"]),
        mesh=mesh, in_specs=in_specs, out_specs=out_specs, check_vma=False,
    )
```

```python
import functools
import math

import jax
import jax.numpy as jnp
import numpy as np
from jax import lax
from jax.experimental import pallas as pl
from jax.experimental.pallas import tpu as pltpu
from jax.sharding import PartitionSpec as P

viscosity = 0.05
time_step = 0.2
keep_weight = -5.0 / 9.0
section_weight = 15.0 / 16.0
shear_param = 1.5
fraction = 0.375
GROUPS = 8
MESH = pl.DeviceIdType.MESH
F32 = jnp.float32
BF16 = jnp.bfloat16


def tables(width_y, depth_z):
    half = width_y // (2 * GROUPS)
    lanes = np.arange(width_y)
    mode = lanes // (2 * half) * half + lanes % half
    is_im = (lanes // half) % 2 == 1
    coarse = np.arange(width_y // half)
    fine = np.arange(half)

    def angle(n, k):
        return 2.0 * np.pi / width_y * ((n[:, None] * k[None, :]) % width_y)

    scale = 1.0 / math.sqrt(width_y)
    alpha = angle(coarse * half, mode)
    beta = angle(fine, mode)
    fwd_coarse = np.concatenate([np.cos(alpha), np.sin(alpha)])
    fwd_fine = scale * np.where(is_im[None], -np.sin(beta), np.cos(beta))
    cells = np.arange(width_y)
    alpha = angle(np.arange(GROUPS) * half, cells)
    beta = angle(fine, cells)
    inv_coarse = np.concatenate([np.cos(alpha), np.sin(alpha)])
    inv_fine = (2.0 * section_weight * scale) * np.stack([np.cos(beta), -np.sin(beta)])
    wave_y = 2.0 * np.pi / width_y * mode[None, :]
    wave_y = np.concatenate([wave_y, np.cos(fraction * wave_y), np.sin(fraction * wave_y)])
    m = np.arange(depth_z)
    signed = np.where(m < depth_z // 2, m, m - depth_z)
    wave_z = (2.0 * np.pi / depth_z * signed)[:, None]
    angle_z = 2.0 * np.pi / depth_z * ((m[:, None] * m[None, :]) % depth_z)
    forward = np.exp(-1j * angle_z) / math.sqrt(depth_z)
    mats = [
        forward,
        1j * wave_z * forward,
        -viscosity * wave_z * wave_z * forward,
        np.exp(1j * angle_z) / math.sqrt(depth_z),
    ]
    stacked = []
    for mat in mats:
        both = np.concatenate([mat.real, mat.imag]).astype(np.float32)
        high = both.astype(BF16)
        low = (both - high.astype(np.float32)).astype(BF16)
        stacked.append(np.concatenate([high, low]))
    as32 = lambda v: jnp.asarray(np.asarray(v, np.float32))
    return (
        as32(fwd_coarse),
        as32(fwd_fine),
        as32(inv_coarse),
        as32(inv_fine),
        as32(wave_y),
        as32(np.broadcast_to(wave_z, (depth_z, 2 * half))),
        jnp.asarray(np.stack(stacked)),
    )


def split(value):
    high = value.astype(BF16)
    low = (value - high.astype(F32)).astype(BF16)
    return high, low


def mm(a, b):
    return jnp.dot(a, b, preferred_element_type=F32)


def body(
    slabs,
    shift_ref,
    vel_hbm,
    qold_hbm,
    guess_hbm,
    fcoarse_hbm,
    ffine_hbm,
    icoarse_hbm,
    ifine_hbm,
    wavey_hbm,
    wavez_hbm,
    zmat_hbm,
    vnext_hbm,
    qnext_hbm,
    pout_hbm,
    ghost,
    relay,
    fcoarse,
    ffine,
    icoarse,
    ifine,
    wavey,
    wavez,
    zmat,
    qold,
    f_hi,
    f_lo,
    left_side,
    spec_u,
    spec_c,
    spec_w,
    got_u,
    got_c,
    got_w,
    tend,
    tend_x,
    cross,
    guess,
    late,
    recip,
    diverge,
    first,
    press,
    spatial,
    got_s,
    load_sem,
    halo_send,
    halo_recv,
    fwd_send,
    fwd_recv,
    inv_send,
    inv_recv,
    out_sem,
):
    gx = lax.axis_index("gx")
    me = lax.axis_index("yz")
    my_z = me // 2
    right = lax.rem(gx + 1, slabs)
    left = lax.rem(gx + slabs - 1, slabs)
    relayed = slabs == 16
    near = 256
    planes = 6
    rows = 24
    width = 1024
    depth = 192
    lanes = 128
    half = 64
    flat = planes * rows * 3

    def peer(d):
        return lax.rem(me + d, GROUPS)

    def own_cols(ref_index):
        return pl.ds(pl.multiple_of(ref_index * lanes, lanes), lanes)

    def own_rows(ref_index):
        return pl.ds(pl.multiple_of(ref_index * rows, 8), rows)

    loads = [
        (vel_hbm, ghost.at[:, pl.ds(3, planes)]),
        (fcoarse_hbm, fcoarse),
        (ffine_hbm, ffine.at[0]),
        (guess_hbm, guess.at[pl.ds(1, planes)]),
        (wavey_hbm, wavey),
        (zmat_hbm, zmat),
        (wavez_hbm, wavez),
        (icoarse_hbm, icoarse),
        (ifine_hbm, ifine),
        (qold_hbm, qold),
    ]
    loads = [pltpu.make_async_copy(s, d, load_sem.at[i]) for i, (s, d) in enumerate(loads)]
    for i in (1, 2, 0, 3, 4, 5, 6, 7, 8, 9):
        loads[i].start()

    barrier = pltpu.get_barrier_semaphore()
    for d in range(1, GROUPS):
        pl.semaphore_signal(
            barrier, inc=1, device_id={"gx": gx, "yz": peer(d)}, device_id_type=MESH
        )
    for side in (left, right):
        pl.semaphore_signal(barrier, inc=1, device_id={"gx": side, "yz": me}, device_id_type=MESH)
    place = lax.rem(gx, 8)
    ends_right = place == 7
    ends_left = place == 0
    helps_left = place == 3
    helps_right = place == 4
    helper = ends_right | ends_left | helps_left | helps_right
    far_side = lax.rem(gx + jnp.where(ends_right | helps_left, 5, slabs - 5), slabs)
    near_side = lax.rem(gx + jnp.where(ends_right | helps_right, slabs - 4, 4), slabs)
    if relayed:

        @pl.when(helper)
        def _():
            for side in (far_side, near_side):
                pl.semaphore_signal(
                    barrier, inc=1, device_id={"gx": side, "yz": me}, device_id_type=MESH
                )

    def x_copy(src, dst, slot, target):
        return pltpu.make_async_remote_copy(
            src_ref=src, dst_ref=dst, send_sem=halo_send.at[slot], recv_sem=halo_recv.at[slot],
            device_id={"gx": target, "yz": me}, device_id_type=MESH,
        )

    def halo(ref, count, slot, lead):
        def at(start):
            return ref.at[:, pl.ds(start, count)] if lead else ref.at[pl.ds(start, count)]

        return (
            x_copy(at(count), at(count + planes), slot, left),
            x_copy(at(planes), at(0), slot + 1, right),
        )

    sign = jnp.where(lax.broadcasted_iota(jnp.int32, (1, lanes), 1) < half, -1.0, 1.0).astype(F32)

    def turned(value):
        return pltpu.roll(value, half, 1) * sign

    def store_split(at, value, gap=flat):
        high, low = split(value)
        left_side[pl.ds(pl.multiple_of(at, 48), 48), :] = high
        left_side[pl.ds(pl.multiple_of(at + gap, 48), 48), :] = low

    def build(col):
        cols = pl.ds(col, 256)
        for side in range(2):
            part = pl.ds(pl.multiple_of(col + side * lanes, lanes), lanes)
            ffine[1, :, part] = -turned(ffine[0, :, part])

        def step(a, carry):
            value = (
                fcoarse[pl.ds(a, 1), cols] * ffine[0, :, cols]
                + fcoarse[pl.ds(a + width // half, 1), cols] * ffine[1, :, cols]
            )
            high, low = split(value)
            where = pl.ds(pl.multiple_of(a * half, half), half)
            f_hi[where, cols] = high
            f_lo[where, cols] = low
            return carry

        lax.fori_loop(0, width // half, step, 0)

    def pairs_loop(write):
        def step(i, carry):
            write(i // 3, lax.rem(i, 3) * 2, i * 48)
            return carry

        lax.fori_loop(0, 9, step, 0)

    def to_modes(slot, col):
        cols = pl.ds(col, 256)
        both = mm(left_side[pl.ds(slot * 2 * flat, 2 * flat), :], f_hi[:, cols])
        low = mm(left_side[pl.ds(slot * 2 * flat, flat), :], f_lo[:, cols])
        return both[:flat] + both[flat:] + low

    def column(i):
        target = lax.rem(my_z + jnp.where(i == 0, 1, jnp.where(i == 1, 3, jnp.where(i == 2, 2, 0))), 4)
        return target, pl.multiple_of(target * 256, 256)

    def fwd_copy(spec, got, kind, dest, at, count):
        return pltpu.make_async_remote_copy(
            src_ref=spec.at[pl.ds(at, count), :, own_cols(dest)],
            dst_ref=got.at[pl.ds(at, count), own_rows(me), :],
            send_sem=fwd_send.at[kind, dest],
            recv_sem=fwd_recv.at[kind, me],
            device_id={"gx": gx, "yz": dest},
            device_id_type=MESH,
        )

    def fwd_own(spec, got, kind, at, count):
        return pltpu.make_async_copy(
            spec.at[pl.ds(at, count), :, own_cols(me)],
            got.at[pl.ds(at, count), own_rows(me), :],
            fwd_recv.at[kind, me],
        )

    def fwd_wait(spec, got, kind, at, count):
        fwd_own(spec, got, kind, at, count).wait()

        def step(d, carry):
            src = peer(d)
            where = got.at[pl.ds(at, count), own_rows(src), :]
            pltpu.make_async_remote_copy(
                src_ref=where, dst_ref=where, send_sem=fwd_send.at[kind, src],
                recv_sem=fwd_recv.at[kind, src], device_id={"gx": gx, "yz": src},
                device_id_type=MESH,
            ).wait_recv()
            return carry

        lax.fori_loop(1, GROUPS, step, 0)

    def send_column(spec, got, kind, i, at, count):
        target, _ = column(i)
        for side in range(2):
            dest = target * 2 + side

            @pl.when(dest != me)
            def _():
                fwd_copy(spec, got, kind, dest, at, count).start()

    def put_u(c, p, at):
        store_split(at, ghost[c, pl.ds(3 + p, 2)].reshape(48, width))

    def modes_of(spec, i, make):
        _, col = column(i)
        if make:
            build(col)
        spec[:, :, pl.ds(col, 256)] = to_modes(0, col).reshape(18, rows, 256)

    loads[1].wait()
    loads[2].wait()
    build(column(0)[1])
    loads[0].wait()
    pairs_loop(put_u)
    modes_of(spec_u, 0, False)
    loads[3].wait()
    vel_halo = halo(ghost, 3, 0, True)
    guess_halo = halo(guess, 1, 2, False)

    def part(ref, start, side):
        cols = pl.ds(0, near) if side == 0 else pl.ds(near, width - near)
        return ref.at[:, pl.ds(start, 3), :, cols]

    near_halo = (
        x_copy(part(ghost, 3, 0), part(ghost, planes + 3, 0), 0, left),
        x_copy(part(ghost, planes, 0), part(ghost, 0, 0), 1, right),
    )
    to_relay = (
        x_copy(part(ghost, 3, 1), relay, 8, far_side),
        x_copy(part(ghost, planes, 1), relay, 8, far_side),
    )
    from_relay = (
        x_copy(relay, part(ghost, planes + 3, 1), 9, near_side),
        x_copy(relay, part(ghost, 0, 1), 9, near_side),
    )

    if relayed:
        pl.semaphore_wait(barrier, jnp.where(helper, GROUPS + 3, GROUPS + 1))
        for i, ends in ((0, ends_left), (1, ends_right)):

            @pl.when(ends)
            def _():
                to_relay[i].start()
                near_halo[i].start()

            @pl.when(jnp.logical_not(ends))
            def _():
                vel_halo[i].start()

    else:
        pl.semaphore_wait(barrier, GROUPS + 1)
        for copy in vel_halo:
            copy.start()
    for copy in guess_halo:
        copy.start()
    send_column(spec_u, got_u, 0, 0, 0, 18)

    def rest_u(i, carry):
        modes_of(spec_u, i, True)
        send_column(spec_u, got_u, 0, i, 0, 18)
        return carry

    lax.fori_loop(1, 4, rest_u, 0)
    fwd_own(spec_u, got_u, 0, 0, 18).start()

    def put_c(c, p, at):
        u_z = ghost[2, pl.ds(3 + p, 2)]
        store_split(at, (-u_z * ghost[c, pl.ds(3 + p, 2)]).reshape(48, width))

    pairs_loop(put_c)

    def all_c(i, carry):
        modes_of(spec_c, i, False)
        send_column(spec_c, got_c, 1, i, 0, 18)
        return carry

    lax.fori_loop(0, 4, all_c, 0)
    fwd_own(spec_c, got_c, 1, 0, 18).start()

    if relayed:
        for i, helps in ((0, helps_left), (1, helps_right)):

            @pl.when(helps)
            def _():
                to_relay[i].wait_recv()
                from_relay[i].start()

        for i, ends in ((0, ends_right), (1, ends_left)):

            @pl.when(ends)
            def _():
                near_halo[i].wait_recv()
                from_relay[i].wait_recv()

            @pl.when(jnp.logical_not(ends))
            def _():
                vel_halo[i].wait_recv()

    else:
        for copy in vel_halo:
            copy.wait_recv()
    shift = shift_ref[0]

    def fix(start, amount, extra):
        def step(i, carry):
            c, p = i // 3, lax.rem(i, 3) + start
            once = pltpu.roll(ghost[c, p], amount, 1)
            ghost[c, p] = (1.0 - fraction) * once + fraction * pltpu.roll(once, extra, 1)
            return carry

        lax.fori_loop(0, 9, step, 0)

    @pl.when(gx == 0)
    def _():
        fix(0, lax.rem(width - shift, width), width - 1)

    @pl.when(gx == slabs - 1)
    def _():
        fix(planes + 3, shift, 1)

    total_x = planes * slabs
    omega = 2.0 / total_x

    def put_ab(i, carry):
        c, p = i // 3, lax.rem(i, 3) * 2
        terms_a = []
        terms_b = []
        for q in range(2):
            at = p + q + 3
            u_x = [ghost[0, at + o] for o in range(-3, 4)]
            u_i = [ghost[c, at + o] for o in range(-3, 4)]
            prod = [x * y for x, y in zip(u_x, u_i)]
            slope = (
                (45.0 / 60.0) * (prod[4] - prod[2])
                - (9.0 / 60.0) * (prod[5] - prod[1])
                + (1.0 / 60.0) * (prod[6] - prod[0])
            )
            bend = (
                (2.0 / 180.0) * (u_i[6] + u_i[0])
                - (27.0 / 180.0) * (u_i[5] + u_i[1])
                + (270.0 / 180.0) * (u_i[4] + u_i[2])
                - (490.0 / 180.0) * u_i[3]
            )
            u_y = ghost[1, at]
            weight_y = jnp.where(c == 0, 2.0 * omega, 0.0).astype(F32)
            weight_x = jnp.where(c == 1, -(2.0 - shear_param) * omega, 0.0).astype(F32)
            terms_a.append(viscosity * bend - slope + (weight_y * u_y + weight_x * u_x[3]))
            place = (gx * planes + p + q).astype(F32) + 0.5 - total_x / 2.0
            background = -shear_param * omega * place
            terms_b.append(-(u_y + background) * u_i[3])
        store_split(i * 48, jnp.concatenate(terms_a, axis=0))
        store_split(2 * flat + i * 48, jnp.concatenate(terms_b, axis=0))
        return carry

    lax.fori_loop(0, 9, put_ab, 0)
    loads[4].wait()

    def combine(i, carry):
        _, col = column(i)
        ya = to_modes(0, col)
        yb = to_modes(1, col)
        for side in range(2):
            wide = pl.ds(pl.multiple_of(col + side * lanes, lanes), lanes)
            cut = slice(side * lanes, (side + 1) * lanes)
            ky = wavey[0:1, wide]
            yu = spec_u[:, :, wide].reshape(flat, lanes)
            out = ya[:, cut] + turned(yb[:, cut]) * ky - (viscosity * ky * ky) * yu
            spec_w[:, :, wide] = out.reshape(18, rows, lanes)
        return carry

    lax.fori_loop(0, 4, combine, 0)
    w_parts = ((2, 0, 6), (3, 6, 6), (4, 12, 2), (5, 14, 2), (6, 16, 2))
    for kind, at, count in w_parts:
        def send_w(i, carry, kind=kind, at=at, count=count):
            send_column(spec_w, got_w, kind, i, at, count)
            return carry

        lax.fori_loop(0, 4, send_w, 0)
        fwd_own(spec_w, got_w, kind, at, count).start()

    for i in (5, 6, 7, 8):
        loads[i].wait()
    own_ky = wavey[0:1, own_cols(me)]
    recip[...] = 1.0 / (2.0 + own_ky * own_ky + wavez[...] * wavez[...])

    def build_back(g, carry):
        cosine = icoarse[pl.ds(g, 1), :]
        sine = icoarse[pl.ds(g + GROUPS, 1), :]
        for part in range(2):
            if part == 0:
                value = cosine * ifine[0] + sine * ifine[1]
            else:
                value = cosine * ifine[1] - sine * ifine[0]
            high, low = split(value)
            where = pl.ds(pl.multiple_of(g * lanes + part * half, half), half)
            f_hi[where, :] = high
            f_lo[where, :] = low
        return carry

    lax.fori_loop(0, GROUPS, build_back, 0)
    top = lax.broadcasted_iota(jnp.int32, (16, width), 0) == 0
    for table in (f_hi, f_lo):
        lines = table[0:16, :].astype(F32)
        table[0:16, :] = jnp.where(top, lines * 0.5, lines).astype(BF16)

    own = own_cols(me)
    coarse = shift // half
    fine = lax.rem(shift, half)
    real_lane = lax.broadcasted_iota(jnp.int32, (1, lanes), 1) < half

    def row_of(lines, row):
        there = lax.broadcasted_iota(jnp.int32, lines.shape, 0) == row
        return jnp.sum(jnp.where(there, lines, 0.0), axis=0, keepdims=True)

    first_row = row_of(ffine[0, :, own], fine)
    second_row = row_of(ffine[1, :, own], fine)
    unit = math.sqrt(width)
    cos_b = unit * jnp.where(real_lane, first_row, -second_row)
    sin_b = -unit * jnp.where(real_lane, second_row, first_row)
    cos_c, sin_c = wavey[1:2, own], wavey[2:3, own]
    cos_b, sin_b = cos_b * cos_c - sin_b * sin_c, sin_b * cos_c + cos_b * sin_c
    cos_c = row_of(fcoarse[0 : width // half, own], coarse)
    sin_c = row_of(fcoarse[width // half : 2 * width // half, own], coarse)
    cosine = cos_b * cos_c - sin_b * sin_c
    sine = sin_b * cos_c + cos_b * sin_c

    def rotate_ends(lower, upper):
        @pl.when(gx == 0)
        def _():
            for ref, j in lower:
                value = ref[j]
                ref[j] = value * cosine + turned(value) * sine

        @pl.when(gx == slabs - 1)
        def _():
            for ref, j in upper:
                value = ref[j]
                ref[j] = value * cosine - turned(value) * sine

    for copy in guess_halo:
        copy.wait_recv()
    rotate_ends(((guess, 0),), ((guess, planes + 1),))

    def z_pair(ref, at, kind):
        value = jnp.concatenate([ref[at], ref[at + 1]], axis=1)
        high, low = split(value)
        return mm(zmat[kind], high), mm(zmat[kind, pl.ds(0, 2 * depth)], low)

    def z_join(parts):
        total = sum(wide[: 2 * depth] + wide[2 * depth :] + low for wide, low in parts)
        out = []
        for q in range(2):
            cut = slice(q * lanes, (q + 1) * lanes)
            out.append(total[:depth, cut] + turned(total[depth:, cut]))
        return out

    fwd_wait(spec_u, got_u, 0, 0, 18)
    fwd_wait(spec_c, got_c, 1, 0, 18)

    def z_first(i, carry):
        at = i * 2
        values = z_join([z_pair(got_c, at, 1), z_pair(got_u, at, 2)])
        tend[at] = values[0]
        tend[at + 1] = values[1]
        return carry

    lax.fori_loop(0, 9, z_first, 0)

    def z_last(c, pair):
        at = c * planes + pair * 2
        values = z_join([z_pair(got_w, at, 0)])
        for q in range(2):
            value = tend[at + q] + values[q]
            tend[at + q] = value
            values[q] = value
        return values

    fwd_wait(spec_w, got_w, 2, 0, 6)

    def last_x(pair, carry):
        values = z_last(0, pair)
        for q in range(2):
            tend_x[2 * pair + q + 1] = values[q]
        return carry

    lax.fori_loop(0, 3, last_x, 0)
    x_halo = halo(tend_x, 1, 4, False)
    for copy in x_halo:
        copy.start()

    fwd_wait(spec_w, got_w, 3, 6, 6)

    def last_y(pair, carry):
        values = z_last(1, pair)
        for q in range(2):
            cross[2 * pair + q] = turned(values[q]) * own_ky
        return carry

    lax.fori_loop(0, 3, last_y, 0)

    def last_z(pair, carry):
        fwd_wait(spec_w, got_w, 4 + pair, 12 + 2 * pair, 2)
        values = z_last(2, pair)
        for q in range(2):
            j = 2 * pair + q
            cross[j] = cross[j] + turned(values[q]) * wavez[...]
        return carry

    lax.fori_loop(0, 3, last_z, 0)

    def sweep_own(j):
        diverge[j + 1] = 0.5 * (tend_x[j + 2] - tend_x[j]) + cross[j]
        first[j + 1] = (guess[j + 2] + guess[j] - diverge[j + 1]) * recip[...]

    for j in (1, 4):
        sweep_own(j)
    low = 0.5 * tend_x[2] + cross[0]
    high = 0.5 * tend_x[5] - cross[5]
    late[0] = guess[2] - low
    late[1] = first[2] - low
    late[2] = guess[5] + high
    late[3] = first[5] + high
    late_halo = (
        x_copy(late.at[pl.ds(0, 2)], late.at[pl.ds(6, 2)], 6, left),
        x_copy(late.at[pl.ds(2, 2)], late.at[pl.ds(4, 2)], 7, right),
    )
    for copy in late_halo:
        copy.start()
    for copy in x_halo:
        copy.wait_recv()
    rotate_ends(((tend_x, 0),), ((tend_x, planes + 1),))
    for j in (0, 2, 3, 5):
        sweep_own(j)

    def sweep_again(j):
        press[j + 1] = (first[j + 2] + first[j] - diverge[j + 1]) * recip[...]

    for j in (1, 2, 3, 4):
        sweep_again(j)
    loads[9].wait()

    def inv_copy(pair, c, dest):
        at = pair * 6 + c * 2
        return pltpu.make_async_remote_copy(
            src_ref=spatial.at[pl.ds(at, 2), own_rows(dest), :],
            dst_ref=got_s.at[pl.ds(at, 2), :, own_cols(me)],
            send_sem=inv_send.at[pair * 3 + c, dest],
            recv_sem=inv_recv.at[pair * 3 + c, me],
            device_id={"gx": gx, "yz": dest},
            device_id_type=MESH,
        )

    def inv_own(pair, c):
        at = pair * 6 + c * 2
        return pltpu.make_async_copy(
            spatial.at[pl.ds(at, 2), own_rows(me), :],
            got_s.at[pl.ds(at, 2), :, own_cols(me)],
            inv_recv.at[pair * 3 + c, me],
        )

    def finish(pair):
        for q in range(2):
            p = 2 * pair + q
            here = press[p + 1]
            side = turned(here)
            slopes = (0.5 * (press[p + 2] - press[p]), side * own_ky, side * wavez[...])
            for c in range(3):
                qold[c, p] = keep_weight * qold[c, p] + time_step * (
                    tend[c * planes + p] - slopes[c]
                )

        def back(c, carry):
            at = pair * 6 + c * 2
            values = z_join([z_pair(qold.at[c], 2 * pair, 3)])
            spatial[at] = values[0]
            spatial[at + 1] = values[1]

            def send(d, inner):
                inv_copy(pair, c, peer(d)).start()
                return inner

            lax.fori_loop(1, GROUPS, send, 0)
            inv_own(pair, c).start()
            return carry

        lax.fori_loop(0, 3, back, 0)

    finish(1)
    for copy in late_halo:
        copy.wait_recv()
    rotate_ends(((late, 4), (late, 5)), ((late, 6), (late, 7)))
    low = 0.5 * tend_x[1]
    first[0] = (guess[1] + late[4] - low) * recip[...]
    press[0] = (first[1] + late[5] - low) * recip[...]
    high = 0.5 * tend_x[6]
    first[7] = (guess[6] + late[6] + high) * recip[...]
    press[7] = (first[6] + late[7] + high) * recip[...]
    for j in (0, 5):
        sweep_again(j)

    def finish_ends(i, carry):
        finish(i * 2)
        return carry

    lax.fori_loop(0, 2, finish_ends, 0)

    def result(c, pair, slot):
        return pltpu.make_async_copy(
            spec_u.at[pl.ds(pair * 6 + 2 * c, 2)], vnext_hbm.at[c, pl.ds(2 * pair, 2)], out_sem.at[slot]
        )

    results = [
        pltpu.make_async_copy(press.at[pl.ds(1, planes)], pout_hbm, out_sem.at[0]),
        pltpu.make_async_copy(qold, qnext_hbm, out_sem.at[1]),
    ]
    for copy in results:
        copy.start()
    results += [result(c, pair, 2 + pair * 3 + c) for pair in range(3) for c in range(3)]

    def sent_u(d, carry):
        dest = peer(d)
        fwd_copy(spec_u, got_u, 0, dest, 0, 18).wait_send()
        fwd_copy(spec_c, got_c, 1, dest, 0, 18).wait_send()
        for kind, at, count in w_parts:
            fwd_copy(spec_w, got_w, kind, dest, at, count).wait_send()
        return carry

    lax.fori_loop(1, GROUPS, sent_u, 0)

    rows_c = 2 * rows

    def arrive(i, carry):
        c = lax.rem(i, 3)
        pair = jnp.where(i < 3, 1, jnp.where(i < 6, 0, 2))
        at = pair * 6 + c * 2
        inv_own(pair, c).wait()

        def step(d, inner):
            src = peer(d)
            where = got_s.at[pl.ds(at, 2), :, own_cols(src)]
            pltpu.make_async_remote_copy(
                src_ref=where, dst_ref=where, send_sem=inv_send.at[pair * 3 + c, src],
                recv_sem=inv_recv.at[pair * 3 + c, src], device_id={"gx": gx, "yz": src},
                device_id_type=MESH,
            ).wait_recv()
            return inner

        lax.fori_loop(1, GROUPS, step, 0)
        high, low = split(got_s[pl.ds(at, 2)].reshape(rows_c, width))
        left_side[0:rows_c, :] = high
        left_side[rows_c : 2 * rows_c, :] = low

        def cells(k, inner):
            cols = pl.ds(pl.multiple_of(k * 512, 512), 512)
            both = mm(left_side[0 : 2 * rows_c, :], f_hi[:, cols])
            out = both[:rows_c] + both[rows_c:] + mm(left_side[0:rows_c, :], f_lo[:, cols])
            spec_u[pl.ds(at, 2), :, cols] = (
                ghost[c, pl.ds(3 + 2 * pair, 2), :, cols] + out.reshape(2, rows, 512)
            )
            return inner

        lax.fori_loop(0, 2, cells, 0)
        result(c, pair, 2 + pair * 3 + c).start()
        return carry

    lax.fori_loop(0, 9, arrive, 0)

    def drain(d, carry):
        dest = peer(d)
        for pair in range(3):
            for c in range(3):
                inv_copy(pair, c, dest).wait_send()
        return carry

    lax.fori_loop(1, GROUPS, drain, 0)
    if relayed:
        for i, ends, helps in ((0, ends_left, helps_left), (1, ends_right, helps_right)):

            @pl.when(ends)
            def _():
                to_relay[i].wait_send()
                near_halo[i].wait_send()

            @pl.when(jnp.logical_not(ends))
            def _():
                vel_halo[i].wait_send()

            @pl.when(helps)
            def _():
                from_relay[i].wait_send()

    else:
        for copy in vel_halo:
            copy.wait_send()
    for copy in guess_halo + x_halo + late_halo:
        copy.wait_send()
    for copy in results:
        copy.wait()


def move(*refs):
    v_in, q_in, p_in, v_out, q_out, p_out, v, q, p, sem_in, sem_out = refs
    legs = []
    for c in range(3):
        legs.append((v_in.at[c], v.at[c], v_out.at[c]))
        legs.append((q_in.at[c], q.at[c], q_out.at[c]))
    legs.append((p_in, p, p_out))
    into = [pltpu.make_async_copy(a, b, sem_in.at[i]) for i, (a, b, _) in enumerate(legs)]
    out = [pltpu.make_async_copy(b, c, sem_out.at[i]) for i, (_, b, c) in enumerate(legs)]
    for copy in into:
        copy.start()
    for first, second in zip(into, out):
        first.wait()
        second.start()
    for copy in out:
        copy.wait()


def local(slabs, vel, q_old, pressure_guess, shear_shift):
    width = vel.shape[3]
    depth = q_old.shape[2]
    half = width // (2 * GROUPS)
    planes, rows = vel.shape[1], vel.shape[2]
    consts = tables(width, depth)
    any_spec = pl.BlockSpec(memory_space=pl.ANY)
    vmem = lambda *shape: pltpu.VMEM(shape, F32)
    wide = lambda n: pltpu.VMEM((n, depth, 2 * half), F32)
    flat = 3 * planes * rows
    scratch = [
        vmem(3, planes + 6, rows, width),
        vmem(3, 3, rows, width - 256),
        vmem(*consts[0].shape),
        vmem(2, *consts[1].shape),
        vmem(*consts[2].shape),
        vmem(*consts[3].shape),
        vmem(*consts[4].shape),
        vmem(*consts[5].shape),
        pltpu.VMEM(consts[6].shape, BF16),
        vmem(3, planes, depth, 2 * half),
        pltpu.VMEM((width, width), BF16),
        pltpu.VMEM((width, width), BF16),
        pltpu.VMEM((4 * flat, width), BF16),
        vmem(3 * planes, rows, width),
        vmem(3 * planes, rows, width),
        vmem(3 * planes, rows, width),
        wide(3 * planes),
        wide(3 * planes),
        wide(3 * planes),
        wide(3 * planes),
        wide(planes + 2),
        wide(planes),
        wide(planes + 2),
        wide(8),
        vmem(depth, 2 * half),
        wide(planes + 2),
        wide(planes + 2),
        wide(planes + 2),
        wide(3 * planes),
        vmem(3 * planes, rows, width),
        pltpu.SemaphoreType.DMA((10,)),
        pltpu.SemaphoreType.DMA((10,)),
        pltpu.SemaphoreType.DMA((10,)),
        pltpu.SemaphoreType.DMA((7, GROUPS)),
        pltpu.SemaphoreType.DMA((7, GROUPS)),
        pltpu.SemaphoreType.DMA((9, GROUPS)),
        pltpu.SemaphoreType.DMA((9, GROUPS)),
        pltpu.SemaphoreType.DMA((11,)),
    ]
    call = pl.pallas_call(
        functools.partial(body, slabs),
        out_shape=(
            jax.ShapeDtypeStruct(vel.shape, F32),
            jax.ShapeDtypeStruct(q_old.shape, F32),
            jax.ShapeDtypeStruct(pressure_guess.shape, F32),
        ),
        in_specs=[pl.BlockSpec(memory_space=pltpu.SMEM)] + [any_spec] * 10,
        out_specs=(any_spec, any_spec, any_spec),
        scratch_shapes=scratch,
        compiler_params=pltpu.CompilerParams(
            collective_id=0, has_side_effects=True, vmem_limit_bytes=63 * 2**20
        ),
        name="section",
    )
    out = call(shear_shift, vel, q_old, pressure_guess, *consts)
    return pl.pallas_call(
        move,
        out_shape=tuple(jax.ShapeDtypeStruct(v.shape, F32) for v in out),
        in_specs=[any_spec] * 3,
        out_specs=(any_spec, any_spec, any_spec),
        scratch_shapes=[pltpu.VMEM(v.shape, F32) for v in out]
        + [pltpu.SemaphoreType.DMA((7,)), pltpu.SemaphoreType.DMA((7,))],
        compiler_params=pltpu.CompilerParams(vmem_limit_bytes=63 * 2**20),
        name="move",
    )(*out)


def solution(mesh):
    in_specs = (P(None, "gx", "yz", None), P(None, "gx", None, "yz"), P("gx", None, "yz"), P())
    out_specs = (P(None, "gx", "yz", None), P(None, "gx", None, "yz"), P("gx", None, "yz"))
    return jax.shard_map(
        functools.partial(local, mesh.shape["gx"]),
        mesh=mesh, in_specs=in_specs, out_specs=out_specs, check_vma=False,
    )
```
